256 devices in a mesh: gx: 32 (over z_hi, y, core), gy: 8 (over x, z_lo).
Axes of the slice: x: 4, y: 4, z: 8 (z_hi: 4, z_lo: 2; z = z_hi * 2 + z_lo), core: 2. Of those that a mesh axis runs over, the one named last changes fastest.
Arguments:
- state: float32 [12, 256, 16, 2048], P(None, 'gx', None, 'gy'), may hold values from -0.9 to 1, as said below
- tissue_mask: int32 [256, 16, 16], P('gx', None, 'gy'), may hold values 0 or 1
- layer_index: int32 [16], replicated, may hold values from 0 to 7
- fibre: float32 [2, 8], replicated, may hold values from -1.2 to 1.2
Outputs:
- new_state: float32 [12, 256, 16, 2048], P(None, 'gx', None, 'gy')
The draws below stay inside these ranges and needn't reach their ends.
Inputs may be any that keep to these rules, and one draw needn't show every extreme that they name: `state`: component 0 lies within -0.9 to 0.3, components 1 to 10 within 0 to 1, component 11 within 0.05 to 1.
All inputs are finite; a program needn't handle non-finite values.
Results may differ from the reference program's by a relative error of at most 0.00002.
Values sent between devices are 32-bit elements.
No kernel may reach another device: no remote copies, remote signals or barrier semaphores. Data moves between devices by JAX's collectives and lax.ppermute only.
A program may use at most 64 MiB of HBM per device.

```python
import math
import jax
import jax.numpy as jnp
from jax import lax

NZ = 16
STEPS = 8
LAYERS = 8
COMPS = 12
MASK_BLOCK = 128
NX = 256
NY = 2048


def draw_state(key, part):
    keys = jax.random.split(jax.random.fold_in(key, 17), 3)
    gates_shape = (COMPS - 2, NX, NZ, NY)
    cell_shape = (1, NX, NZ, NY)
    voltage = jax.random.uniform(keys[0], cell_shape, jnp.float32, -0.9, 0.3)
    gates = jax.random.uniform(keys[1], gates_shape, jnp.float32)
    calcium = 0.05 * 20.0 ** jax.random.uniform(keys[2], cell_shape, jnp.float32)
    return jnp.concatenate([voltage, gates, calcium], axis=0).astype(jnp.float32)


def place_ends(values, key, least, largest):
    index_at = [jax.random.randint(jax.random.fold_in(key, axis), (), 0, length) for axis, length in enumerate(values.shape)]
    longest = values.shape.index(max(values.shape))
    beside = index_at[:longest] + [(index_at[longest] + 1) % values.shape[longest]] + index_at[longest + 1:]
    return values.at[tuple(index_at)].set(least).at[tuple(beside)].set(largest)


def setup_inputs(seed: int = 0) -> dict:
    streams_of = jax.random.split(jax.random.key(seed), 5)
    return {
        "state": draw_state(jax.random.fold_in(streams_of[4], 71), 0),
        "tissue_mask": place_ends((jax.random.randint(streams_of[1], (NX, NZ, NY // MASK_BLOCK), 0, 4) < 3).astype(jnp.int32), jax.random.fold_in(streams_of[1], 1), 0, 1),
        "layer_index": place_ends(jax.random.randint(streams_of[2], (NZ,), 0, LAYERS), jax.random.fold_in(streams_of[2], 1), 0, LAYERS - 1).astype(jnp.int32),
        "fibre": jnp.clip(jax.random.uniform(streams_of[3], (2, LAYERS), jnp.float32, -1.2, 1.2), -1.2, 1.2),
    }


time_step = 0.02
thermal_volt = 8314.472 * 310.0 / 96485.3415
potassium_out = 5.4
sodium_out = 140.0
calcium_out = 2.0
potassium_in = 138.3
sodium_in = 7.67
transverse = 0.04
longitudinal = 0.12

def settle(gate, steady, tau):
    return steady + (gate - steady) * jnp.exp(-time_step / tau)

def settle_rate(gate, steady, rate):
    return steady + (gate - steady) * jnp.exp(-time_step * rate)

def membrane(state):
    sig = jax.nn.sigmoid
    voltage = 100.0 * state[0]
    sodium_act = state[1]
    sodium_inact = state[2]
    sodium_slow = state[3]
    calcium_act = state[4]
    calcium_inact = state[5]
    transient_act = state[6]
    transient_inact = state[7]
    rapid_act = state[8]
    rapid_inact = state[9]
    slow_act = state[10]
    calcium = state[11]
    calcium_mm = jnp.maximum(calcium, 0.02) * 0.001
    rev_potassium = thermal_volt * math.log(potassium_out / potassium_in)
    rev_sodium = thermal_volt * math.log(sodium_out / sodium_in)
    rev_slow = thermal_volt * math.log((potassium_out + 0.03 * sodium_out) / (potassium_in + 0.03 * sodium_in))
    rev_calcium = 0.5 * thermal_volt * jnp.log(calcium_out / calcium_mm)
    sodium_current = 14.838 * sodium_act ** 3 * sodium_inact * sodium_slow * (voltage - rev_sodium)
    calcium_current = 0.08 * calcium_act * calcium_inact * (voltage - rev_calcium)
    transient_current = 0.294 * transient_act * transient_inact * (voltage - rev_potassium)
    rapid_current = 0.153 * rapid_act * rapid_inact * (voltage - rev_potassium)
    slow_current = 0.392 * slow_act ** 2 * (voltage - rev_slow)
    above = voltage - rev_potassium
    alpha_inward = 0.1 * sig(-0.06 * (above - 200.0))
    beta_inward = (3.0 * jnp.exp(0.0002 * (above + 100.0)) + jnp.exp(0.1 * (above - 10.0))) * sig(0.5 * above)
    inward_current = 5.405 * alpha_inward / (alpha_inward + beta_inward) * above
    plateau_current = 0.0146 * sig((voltage - 25.0) / 5.98) * above
    scaled = voltage / thermal_volt
    pump_current = 2.724 * potassium_out / (potassium_out + 1.0) * sodium_in / (sodium_in + 40.0) / (1.0 + 0.1245 * jnp.exp(-0.1 * scaled) + 0.0353 * jnp.exp(-scaled))
    exchange_current = 1000.0 * (jnp.exp(0.35 * scaled) * sodium_in ** 3 * calcium_out - 2.5 * jnp.exp(-0.65 * scaled) * sodium_out ** 3 * calcium_mm) / ((87.5 ** 3 + sodium_out ** 3) * (1.38 + calcium_out) * (1.0 + 0.1 * jnp.exp(-0.65 * scaled)))
    pump_calcium = 0.1238 * calcium_mm / (calcium_mm + 0.0005)
    back_sodium = 0.00029 * (voltage - rev_sodium)
    back_calcium = 0.000592 * (voltage - rev_calcium)
    ionic_total = sodium_current + calcium_current + transient_current + rapid_current + slow_current + inward_current + plateau_current + pump_current + exchange_current + pump_calcium + back_sodium + back_calcium
    new_voltage = voltage - time_step * ionic_total
    new_calcium = calcium - time_step * 0.05 * (calcium_current + back_calcium + pump_calcium - 2.0 * exchange_current)
    upper = sig((voltage + 40.0) / 2.0)
    lower = sig(-(voltage + 40.0) / 2.0)
    tau_act = sig((voltage + 60.0) / 5.0) * (0.1 * sig(-(voltage + 35.0) / 5.0) + 0.1 * sig(-(voltage - 50.0) / 200.0))
    new_act = settle(sodium_act, sig((voltage + 56.86) / 9.03) ** 2, tau_act)
    inact_steady = sig(-(voltage + 71.55) / 7.43) ** 2
    rate_inact = lower * 0.057 * jnp.exp(-(voltage + 80.0) / 6.8) + upper * (0.77 / 0.13) * sig((voltage + 10.66) / 11.1) + lower * (2.7 * jnp.exp(0.079 * voltage) + 310000.0 * jnp.exp(0.3485 * voltage))
    new_inact = settle_rate(sodium_inact, inact_steady, rate_inact)
    rate_slow = lower * (-25428.0 * jnp.exp(0.2444 * voltage) - 6.948e-06 * jnp.exp(-0.04391 * voltage)) * (voltage + 37.78) * sig(-0.311 * (voltage + 79.23)) + lower * 0.02424 * jnp.exp(-0.01052 * voltage) * sig(0.1378 * (voltage + 40.14)) + upper * 0.6 * jnp.exp(0.057 * voltage) * sig(0.1 * (voltage + 32.0))
    new_slow = settle_rate(sodium_slow, inact_steady, rate_slow)
    tau_calact = (1.4 * sig((voltage + 35.0) / 13.0) + 0.25) * 1.4 * sig(-(voltage + 5.0) / 5.0) + sig((voltage - 50.0) / 20.0)
    new_calact = settle(calcium_act, sig((voltage + 8.0) / 7.5), tau_calact)
    tau_calinact = 1102.5 * jnp.exp(-(voltage + 27.0) ** 2 / 225.0) + 200.0 * sig((voltage - 13.0) / 10.0) + 180.0 * sig(-(voltage + 30.0) / 10.0) + 20.0
    new_calinact = settle(calcium_inact, sig(-(voltage + 20.0) / 7.0), tau_calinact)
    tau_tract = 9.5 * jnp.exp(-(voltage + 40.0) ** 2 / 1800.0) + 0.8
    new_tract = settle(transient_act, sig((voltage - 20.0) / 6.0), tau_tract)
    tau_trinact = 85.0 * jnp.exp(-(voltage + 45.0) ** 2 / 320.0) + 5.0 * sig(-(voltage - 20.0) / 5.0) + 3.0
    new_trinact = settle(transient_inact, sig(-(voltage + 20.0) / 5.0), tau_trinact)
    tau_rapact = 450.0 * sig((voltage + 45.0) / 10.0) * 6.0 * sig(-(voltage + 30.0) / 11.5)
    new_rapact = settle(rapid_act, sig((voltage + 26.0) / 7.0), tau_rapact)
    tau_rapinact = 3.0 * sig((voltage + 60.0) / 20.0) * 1.12 * sig(-(voltage - 60.0) / 20.0)
    new_rapinact = settle(rapid_inact, sig(-(voltage + 88.0) / 24.0), tau_rapinact)
    tau_slowact = 1400.0 * jnp.sqrt(sig((voltage - 5.0) / 6.0)) * sig(-(voltage - 35.0) / 15.0) + 80.0
    new_slowact = settle(slow_act, sig((voltage + 5.0) / 14.0), tau_slowact)
    return jnp.stack([new_voltage / 100.0, new_act, new_inact, new_slow, new_calact, new_calinact, new_tract, new_trinact, new_rapact, new_rapinact, new_slowact, new_calcium])

def advance(state, inside):
    return jnp.where(inside[None], membrane(state), state)

def layer_tensor(layer_index, fibre):
    angle_in = fibre[0]
    angle_out = fibre[1]
    fibre_x = jnp.cos(angle_in) * jnp.cos(angle_out)
    fibre_y = jnp.sin(angle_in) * jnp.cos(angle_out)
    fibre_z = jnp.sin(angle_out)
    spread = longitudinal - transverse
    tensor_table = jnp.stack([transverse + spread * fibre_x * fibre_x, transverse + spread * fibre_y * fibre_y, transverse + spread * fibre_z * fibre_z, spread * fibre_x * fibre_y, spread * fibre_x * fibre_z, spread * fibre_y * fibre_z])
    layer_ids = jnp.arange(fibre.shape[1], dtype=jnp.int32)
    chosen = layer_index[:, None] == layer_ids[None, :]
    return lax.optimization_barrier(jnp.sum(jnp.where(chosen[None], tensor_table[:, None, :], jnp.float32(0.0)), axis=2))

def weights(tensor, offset_x, offset_y, offset_z):
    if offset_z == 0:
        if offset_x != 0 and offset_y != 0:
            return offset_x * offset_y * tensor[3] / 2.0
        if offset_x != 0:
            return tensor[0]
        return tensor[1]
    extent_z = tensor.shape[1]
    padded_tensor = jnp.pad(tensor, ((0, 0), (1, 1)), mode='edge')
    averaged = (tensor + padded_tensor[:, 1 + offset_z:1 + offset_z + extent_z]) / 2.0
    if offset_x == 0 and offset_y == 0:
        return averaged[2]
    if offset_x != 0:
        return offset_x * offset_z * averaged[4] / 2.0
    return offset_y * offset_z * averaged[5] / 2.0

def stencil(volt_shell, mask_shell, tensor):
    volt_padded = jnp.pad(volt_shell, ((0, 0), (1, 1), (0, 0)))
    mask_padded = jnp.pad(mask_shell, ((0, 0), (1, 1), (0, 0)))
    extent_x = volt_shell.shape[0] - 2
    extent_z = volt_shell.shape[1]
    extent_y = volt_shell.shape[2] - 2
    centre = volt_padded[1:1 + extent_x, 1:1 + extent_z, 1:1 + extent_y]
    mask_centre = mask_padded[1:1 + extent_x, 1:1 + extent_z, 1:1 + extent_y]
    flux_sum = jnp.zeros_like(centre)
    for offset_x in (-1, 0, 1):
        for offset_y in (-1, 0, 1):
            for offset_z in (-1, 0, 1):
                length = offset_x * offset_x + offset_y * offset_y + offset_z * offset_z
                if length == 0 or length > 2:
                    continue
                weight = weights(tensor, offset_x, offset_y, offset_z)[None, :, None]
                neighbour = volt_padded[1 + offset_x:1 + offset_x + extent_x, 1 + offset_z:1 + offset_z + extent_z, 1 + offset_y:1 + offset_y + extent_y]
                mask_near = mask_padded[1 + offset_x:1 + offset_x + extent_x, 1 + offset_z:1 + offset_z + extent_z, 1 + offset_y:1 + offset_y + extent_y]
                flux_sum = flux_sum + weight * mask_near * (neighbour - centre)
    return mask_centre * flux_sum

def expand_mask(blocks):
    cells_x, extent_z, block_count = blocks.shape
    spread = jnp.broadcast_to(blocks[:, :, :, None], (cells_x, extent_z, block_count, MASK_BLOCK))
    return spread.reshape(cells_x, extent_z, block_count * MASK_BLOCK) > 0

def reference(state, tissue_mask, layer_index, fibre):
    tensor = layer_tensor(layer_index, fibre)
    inside = expand_mask(tissue_mask)
    mask_shell = jnp.pad(inside.astype(jnp.float32), ((1, 1), (0, 0), (1, 1)))
    column_state = jnp.moveaxis(state, 1, 0)
    for repeat in range(STEPS):
        reacted = lax.map(lambda paired: advance(paired[0], paired[1]), (column_state, inside))
        voltage = reacted[:, 0]
        volt_shell = jnp.pad(voltage, ((1, 1), (0, 0), (1, 1)))
        column_state = reacted.at[:, 0].set(voltage + stencil(volt_shell, mask_shell, tensor))
    return jnp.moveaxis(column_state, 0, 1)
```

```python
import functools
import math

import jax
import jax.numpy as jnp
from jax import lax
from jax.experimental import pallas as pl
from jax.experimental.pallas import tpu as pltpu
from jax.sharding import PartitionSpec as P

STEPS = 8
MASK_BLOCK = 128
COMPS = 12
EDGE = 8
GROUP = 2 * EDGE
LANES = 128

time_step = 0.02
thermal_volt = 8314.472 * 310.0 / 96485.3415
potassium_out = 5.4
sodium_out = 140.0
calcium_out = 2.0
potassium_in = 138.3
sodium_in = 7.67
transverse = 0.04
longitudinal = 0.12
LOG2E = math.log2(math.e)


def react(state):
    (x, act, inact, slow, calact, calinact, tract, trinact, rapact, rapinact, slowact, calcium) = state

    def power(rate, offset=0.0, scale=1.0):
        shift = offset * LOG2E + math.log2(scale)
        scaled = x * (100.0 * rate * LOG2E)
        return jnp.exp2(scaled + shift if shift else scaled)

    def bell(centre, width, scale):
        root = math.sqrt(LOG2E / width)
        away = x * (100.0 * root) + centre * root
        return jnp.exp2(math.log2(scale) - away * away)

    def inverse(value):
        return 1.0 / value

    def moved(gate, steady, exponent):
        return steady + (gate - steady) * jnp.exp2(exponent)

    e = math.exp
    decay = -time_step * LOG2E
    voltage = 100.0 * x
    rev_potassium = thermal_volt * math.log(potassium_out / potassium_in)
    rev_sodium = thermal_volt * math.log(sodium_out / sodium_in)
    rev_slow = thermal_volt * math.log((potassium_out + 0.03 * sodium_out) / (potassium_in + 0.03 * sodium_in))
    up20 = power(1 / 20)
    up10 = up20 * up20
    up5 = up10 * up10
    down20 = power(-1 / 20)
    down10 = down20 * down20
    down5 = down10 * down10
    up15 = power(1 / 15)
    down6 = power(-1 / 6)
    down14 = power(-1 / 14)
    down7 = down14 * down14
    fall = jnp.exp2(jnp.minimum(x * (-50.0 * LOG2E) - 20.0 * LOG2E, 120.0))
    upper = inverse(1.0 + fall)
    lower = fall * upper

    above = voltage - rev_potassium
    cam = jnp.maximum(calcium, 0.02)
    past_calcium = voltage - 0.5 * thermal_volt * math.log(calcium_out / 0.001) + (0.5 * thermal_volt) * jnp.log(cam)
    past_sodium = voltage - rev_sodium
    inward_x = 1.0 + power(0.06, -0.06 * (rev_potassium + 200.0))
    inward_y = 1.0 + fall * e(20.0 + 0.5 * rev_potassium)
    inward_b = power(0.0002, 0.0002 * (100.0 - rev_potassium), 30.0) + up10 * (10.0 * e(-0.1 * rev_potassium - 1.0))
    inward = (5.405 * inward_y) * inverse(inward_y + inward_b * inward_x)
    plateau = 0.0146 * inverse(1.0 + power(-1 / 5.98, 25.0 / 5.98))
    pump = (2.724 * potassium_out / (potassium_out + 1.0) * sodium_in / (sodium_in + 40.0)) * inverse(
        1.0 + power(-0.1 / thermal_volt, 0.0, 0.1245) + power(-1.0 / thermal_volt, 0.0, 0.0353))
    whole = 1000.0 / ((87.5**3 + sodium_out**3) * (1.38 + calcium_out))
    back = power(-0.65 / thermal_volt, 0.0, 0.1)
    exchange = (power(0.35 / thermal_volt, 0.0, whole * sodium_in**3 * calcium_out)
                - back * (cam * (10.0 * 2.5 * 0.001 * whole * sodium_out**3))) * inverse(1.0 + back)
    pump_calcium = (0.1238 * cam) * inverse(cam + 0.5)
    calcium_sum = (0.08 * calact * calinact + 0.000592) * past_calcium
    ionic = (
        (14.838 * act * (act * act) * inact * slow + 0.00029) * past_sodium
        + calcium_sum
        + (0.294 * tract * trinact + 0.153 * rapact * rapinact + inward + plateau) * above
        + (0.392 * slowact * slowact) * (voltage - rev_slow)
        + pump
        + exchange
        + pump_calcium
    )
    new_x = x - (time_step / 100.0) * ionic
    new_calcium = calcium - (time_step * 0.05) * (calcium_sum + pump_calcium - 2.0 * exchange)

    a = up5 * e(7.0)
    b = power(1 / 200, -0.25)
    root = inverse(1.0 + power(-1 / 9.03, -56.86 / 9.03))
    rate = (((1.0 + e(-5.0)) * 10.0 * decay + a * (10.0 * decay)) + down5 * (e(-12.0) * 10.0 * decay)) * (1.0 + b) * inverse(2.0 + a + b)
    new_act = moved(act, root * root, rate)

    root = inverse(1.0 + power(1 / 7.43, 71.55 / 7.43))
    steady = root * root
    rate = lower * (power(-1 / 6.8, -80.0 / 6.8, 0.057 * -decay) + power(0.079, 0.0, 2.7 * -decay) + power(0.3485, 0.0, 310000.0 * -decay)) + (
        upper * (0.77 / 0.13 * -decay)) * inverse(1.0 + power(-1 / 11.1, -10.66 / 11.1))
    new_inact = moved(inact, steady, -rate)
    rate = lower * (
        (power(0.2444, 0.0, 25428.0 * -decay) + power(-0.04391, 0.0, 6.948e-06 * -decay)) * (voltage + 37.78) * inverse(1.0 + power(0.311, 0.311 * 79.23))
        - power(-0.01052, 0.0, 0.02424 * -decay) * inverse(1.0 + power(-0.1378, -0.1378 * 40.14))
    ) - upper * power(0.057, 0.0, 0.6 * -decay) * inverse(1.0 + down10 * e(-3.2))
    new_slow = moved(slow, steady, rate)

    p = 1.0 + power(-1 / 13, -35.0 / 13)
    r = 1.0 + down20 * e(2.5)
    pq = p * (1.0 + up5 * e(1.0))
    rate = (decay * pq) * r * inverse((1.96 + 0.35 * p) * r + pq)
    new_calact = moved(calact, inverse(1.0 + power(-1 / 7.5, -8.0 / 7.5)), rate)

    a = down10 * e(1.3)
    b = up10 * e(3.0)
    den = (1.0 + e(4.3)) + a + b
    rate = (decay * den) * inverse((bell(27.0, 225.0, 1102.5) + 20.0) * den + (380.0 + 200.0 * b + 180.0 * a))
    new_calinact = moved(calinact, down7 * inverse(down7 + e(20.0 / 7)), rate)

    rate = decay * inverse(bell(40.0, 1800.0, 9.5) + 0.8)
    new_tract = moved(tract, inverse(1.0 + down6 * e(20.0 / 6)), rate)

    t = 1.0 + up5 * e(-4.0)
    rate = (decay * t) * inverse((bell(45.0, 320.0, 85.0) + 3.0) * t + 5.0)
    new_trinact = moved(trinact, inverse(1.0 + up5 * e(4.0)), rate)

    rate = (decay / 2700.0 + down10 * (e(-4.5) * decay / 2700.0)) * (1.0 + power(1 / 11.5, 30.0 / 11.5))
    new_rapact = moved(rapact, inverse(1.0 + down7 * e(-26.0 / 7)), rate)

    rate = (1.0 + e(-6.0)) * decay / 3.36 + (up20 + down20) * (e(-3.0) * decay / 3.36)
    new_rapinact = moved(rapinact, inverse(1.0 + power(1 / 24, 88.0 / 24)), rate)

    y = 1.0 + up15 * e(-35.0 / 15)
    rate = (decay * y) * inverse(1400.0 * lax.rsqrt(1.0 + down6 * e(5.0 / 6)) + 80.0 * y)
    new_slowact = moved(slowact, inverse(1.0 + down14 * e(-5.0 / 14)), rate)
    return (new_x, new_act, new_inact, new_slow, new_calact, new_calinact, new_tract, new_trinact, new_rapact, new_rapinact, new_slowact, new_calcium)


def layer_tensor(layer_index, fibre):
    angle_in = fibre[0]
    angle_out = fibre[1]
    fibre_x = jnp.cos(angle_in) * jnp.cos(angle_out)
    fibre_y = jnp.sin(angle_in) * jnp.cos(angle_out)
    fibre_z = jnp.sin(angle_out)
    spread = longitudinal - transverse
    tensor_table = jnp.stack(
        [
            transverse + spread * fibre_x * fibre_x,
            transverse + spread * fibre_y * fibre_y,
            transverse + spread * fibre_z * fibre_z,
            spread * fibre_x * fibre_y,
            spread * fibre_x * fibre_z,
            spread * fibre_y * fibre_z,
        ]
    )
    layer_ids = jnp.arange(fibre.shape[1], dtype=jnp.int32)
    chosen = layer_index[:, None] == layer_ids[None, :]
    return jnp.sum(jnp.where(chosen[None], tensor_table[:, None, :], jnp.float32(0.0)), axis=2)


def level_weights(tensor, lanes):
    between = (tensor[:, 1:] + tensor[:, :-1]) / 2.0
    upward = jnp.pad(between, ((0, 0), (0, 1)))
    downward = jnp.pad(between, ((0, 0), (1, 0)))
    rows = jnp.stack(
        [
            tensor[0],
            tensor[1],
            tensor[3] / 2.0,
            upward[2],
            upward[4] / 2.0,
            upward[5] / 2.0,
            downward[2],
            downward[4] / 2.0,
            downward[5] / 2.0,
        ]
    )
    return jnp.broadcast_to(rows[:, :, None], rows.shape + (lanes,))


def edge_kernel(state_ref, mask_ref, edge_ref):
    depth, width = state_ref.shape[2], state_ref.shape[3]
    cells = state_ref.shape[1]
    lane = lax.broadcasted_iota(jnp.int32, (depth, LANES), 1)

    def packed(first, last):
        total = jnp.zeros((depth, LANES), jnp.float32)
        for i in range(cells):
            joined = jnp.where(lane < EDGE, first(i), last(i))
            turned = pltpu.roll(joined, i * GROUP + EDGE, 1)
            total = jnp.where(lane // GROUP == i, turned, total)
        return total

    def one(c, carry):
        edge_ref[c] = packed(
            lambda i: state_ref[c, i, :, :LANES], lambda i: state_ref[c, i, :, width - LANES :]
        )
        return carry

    lax.fori_loop(0, COMPS, one, 0)
    spread = lambda i, b: jnp.broadcast_to(mask_ref[:, 2 * i + b : 2 * i + b + 1], (depth, LANES))
    edge_ref[COMPS] = packed(lambda i: spread(i, 0), lambda i: spread(i, 1))


def steps_kernel(
    left_hbm,
    state_hbm,
    right_hbm,
    strip_left_ref,
    strip_ref,
    strip_right_ref,
    weight_ref,
    out_hbm,
    main,
    inside,
    total,
    pot,
    dy_ref,
    sy_ref,
    strip,
    strip_inside,
    strip_total,
    strip_pot,
    sems,
):
    cells, depth, width = state_hbm.shape[1:]
    span = 3 * cells
    sides = (0, 1)
    long = 3 * LANES
    copies = [
        pltpu.make_async_copy(source, main.at[:, pl.ds(i * cells, cells)], sems.at[i])
        for i, source in enumerate((left_hbm, state_hbm, right_hbm))
    ]
    for copy in copies:
        copy.start()
    lane = lax.broadcasted_iota(jnp.int32, (depth, LANES), 1)
    first_lane = lane == 0
    last_lane = lane == LANES - 1

    for i, source in enumerate((strip_left_ref, strip_ref, strip_right_ref)):
        part = pl.ds(i * LANES, LANES)
        for side in sides:
            for c in range(COMPS):
                strip[c, side, :, part] = source[side * (COMPS + 1) + c]
            strip_inside[side, :, part] = source[side * (COMPS + 1) + COMPS]
            strip_pot[side, :, part] = source[side * (COMPS + 1) + COMPS]
        codes = source[2 * (COMPS + 1)]
        for x in range(cells):
            for b in range(2):
                value = jnp.broadcast_to(codes[:, 2 * x + b : 2 * x + b + 1], (depth, LANES))
                inside[i * cells + x, :, b * LANES : (b + 1) * LANES] = value
                pot[i * cells + x, :, b * LANES : (b + 1) * LANES] = value

    def shift_row(x, carry):
        block = pl.ds(pl.multiple_of(x // 8 * LANES, LANES), LANES)
        place = lax.rem(x, 8) * GROUP
        before = pltpu.roll(strip_pot[0, :, block], lax.rem(2 * LANES - place - (EDGE - 1), LANES), 1)
        after = pltpu.roll(strip_pot[1, :, block], lax.rem(2 * LANES - 1 - place - EDGE, LANES), 1)
        near, far = pot[x, :, :LANES], pot[x, :, LANES:]
        near_up, far_up = pltpu.roll(near, 1, 1), pltpu.roll(far, 1, 1)
        near_down, far_down = pltpu.roll(near, LANES - 1, 1), pltpu.roll(far, LANES - 1, 1)
        lower = jnp.where(first_lane, before, near_up)
        upper = jnp.where(last_lane, far_down, near_down)
        dy_ref[x, :, :LANES] = upper - lower
        sy_ref[x, :, :LANES] = upper + lower
        lower = jnp.where(first_lane, near_up, far_up)
        upper = jnp.where(last_lane, after, far_down)
        dy_ref[x, :, LANES:] = upper - lower
        sy_ref[x, :, LANES:] = upper + lower
        return carry

    def spread(p, dx, sx, dy, sy, cross, lanes):
        w = [weight_ref[i, :, :lanes] for i in range(9)]
        rising = w[3] * p - w[4] * dx - w[5] * dy
        falling = w[6] * p + w[7] * dx + w[8] * dy
        return (
            w[0] * sx
            + w[1] * sy
            + w[2] * cross
            + pltpu.roll(rising, 1, 0)
            + pltpu.roll(falling, depth - 1, 0)
        )

    def row_spread(x):
        before, after = pot[x - 1], pot[x + 1]
        return spread(
            pot[x], after - before, after + before, dy_ref[x], sy_ref[x], dy_ref[x + 1] - dy_ref[x - 1], width
        )

    def strip_spread(side):
        p = strip_pot[side]
        lower, upper = pltpu.roll(p, 1, 1), pltpu.roll(p, long - 1, 1)
        before, after = pltpu.roll(p, GROUP, 1), pltpu.roll(p, long - GROUP, 1)
        dy = upper - lower
        cross = pltpu.roll(dy, long - GROUP, 1) - pltpu.roll(dy, GROUP, 1)
        return spread(p, after - before, after + before, dy, upper + lower, cross, long)

    lax.fori_loop(0, span, shift_row, 0)

    def total_row(x, carry):
        total[x] = row_spread(x)
        return carry

    lax.fori_loop(1, span - 1, total_row, 0)
    for side in sides:
        strip_total[side] = strip_spread(side)
    for copy in copies:
        copy.wait()

    def react_tile(store, held, place, level, part):
        rows = pl.ds(level * 8, 8)
        old = [store[c, place, rows, part] for c in range(COMPS)]
        live = held[place, rows, part]
        new = react(old)
        new = [jnp.where(live > 0.5, a, b) for a, b in zip(new, old)]
        for c in range(COMPS):
            store[c, place, rows, part] = new[c]
        return live * new[0]

    def step(s, carry):
        for side in sides:
            for level in range(depth // 8):
                for i in range(3):
                    part = pl.ds(i * LANES, LANES)
                    value = react_tile(strip, strip_inside, side, level, part)
                    strip_pot[side, pl.ds(level * 8, 8), part] = value

        def react_row(x, carry):
            for level in range(depth // 8):
                for i in range(2):
                    part = pl.ds(i * LANES, LANES)
                    pot[x, pl.ds(level * 8, 8), part] = react_tile(main, inside, x, level, part)
            return carry

        lax.fori_loop(s, span - s, react_row, 0)
        lax.fori_loop(s, span - s, shift_row, 0)

        def diffuse_row(x, carry):
            u = main[0, x]
            main[0, x] = u + inside[x] * (row_spread(x) - u * total[x])
            return carry

        lax.fori_loop(s + 1, span - 1 - s, diffuse_row, 0)
        for side in sides:
            u = strip[0, side]
            strip[0, side] = u + strip_inside[side] * (strip_spread(side) - u * strip_total[side])
        return carry

    lax.fori_loop(0, STEPS, step, 0)
    copy = pltpu.make_async_copy(main.at[:, pl.ds(cells, cells)], out_hbm, sems.at[0])
    copy.start()
    copy.wait()


def shards(state, tissue_mask, layer_index, fibre):
    comps, cells, depth, width = state.shape
    across, along = lax.axis_size("gx"), lax.axis_size("gy")

    def passed(value, axis, size):
        up = [(i, i + 1) for i in range(size - 1)]
        return lax.ppermute(value, axis, up), lax.ppermute(value, axis, [(j, i) for i, j in up])

    vmem = pl.BlockSpec(memory_space=pltpu.VMEM)
    hbm = pl.BlockSpec(memory_space=pl.ANY)
    from_left, from_right = passed(state, "gx", across)

    blocks = tissue_mask.shape[2]
    codes = (tissue_mask > 0).astype(jnp.float32).transpose(1, 0, 2).reshape(depth, cells * blocks)
    codes = jnp.pad(codes, ((0, 0), (0, LANES - cells * blocks)))
    edge = pl.pallas_call(
        edge_kernel,
        out_shape=jax.ShapeDtypeStruct((comps + 1, depth, LANES), jnp.float32),
        in_specs=[vmem, vmem],
        out_specs=vmem,
        compiler_params=pltpu.CompilerParams(vmem_limit_bytes=32 << 20),
        name="edges",
    )(state, codes)
    edge_before, edge_after = passed(edge, "gy", along)
    outer = lax.broadcasted_iota(jnp.int32, edge.shape, 2) % GROUP < EDGE
    strips = jnp.concatenate(
        [jnp.where(outer, edge_before, edge), jnp.where(outer, edge, edge_after), codes[None]]
    )
    strips_left, strips_right = passed(strips, "gx", across)

    weights = level_weights(layer_tensor(layer_index, fibre), 3 * LANES)
    span = 3 * cells
    plane = pltpu.VMEM((span, depth, width), jnp.float32)
    side_plane = pltpu.VMEM((2, depth, 3 * LANES), jnp.float32)
    return pl.pallas_call(
        steps_kernel,
        out_shape=jax.ShapeDtypeStruct(state.shape, state.dtype),
        in_specs=[hbm, hbm, hbm, vmem, vmem, vmem, vmem],
        out_specs=hbm,
        scratch_shapes=[
            pltpu.VMEM((comps, span, depth, width), jnp.float32),
            plane,
            plane,
            plane,
            plane,
            plane,
            pltpu.VMEM((comps, 2, depth, 3 * LANES), jnp.float32),
            side_plane,
            side_plane,
            side_plane,
            pltpu.SemaphoreType.DMA((3,)),
        ],
        compiler_params=pltpu.CompilerParams(vmem_limit_bytes=48 << 20),
        name="steps",
    )(from_left, state, from_right, strips_left, strips, strips_right, weights)


def solution(mesh):
    placed = (P(None, "gx", None, "gy"), P("gx", None, "gy"), P(), P())
    return jax.shard_map(
        shards, mesh=mesh, in_specs=placed, out_specs=P(None, "gx", None, "gy"), check_vma=False
    )
```

```python
import functools
import math

import jax
import jax.numpy as jnp
from jax import lax
from jax.experimental import pallas as pl
from jax.experimental.pallas import tpu as pltpu
from jax.sharding import PartitionSpec as P

STEPS = 8
MASK_BLOCK = 128
COMPS = 12
EDGE = 8
GROUP = 2 * EDGE
LANES = 128

time_step = 0.02
thermal_volt = 8314.472 * 310.0 / 96485.3415
potassium_out = 5.4
sodium_out = 140.0
calcium_out = 2.0
potassium_in = 138.3
sodium_in = 7.67
transverse = 0.04
longitudinal = 0.12
LOG2E = math.log2(math.e)


def react(state):
    (x, act, inact, slow, calact, calinact, tract, trinact, rapact, rapinact, slowact, calcium) = state

    def power(rate, offset=0.0, scale=1.0):
        shift = offset * LOG2E + math.log2(scale)
        scaled = x * (100.0 * rate * LOG2E)
        return jnp.exp2(scaled + shift if shift else scaled)

    def bell(centre, width, scale):
        root = math.sqrt(LOG2E / width)
        away = x * (100.0 * root) + centre * root
        return jnp.exp2(math.log2(scale) - away * away)

    def inverse(value):
        return 1.0 / value

    def moved(gate, steady, exponent):
        return steady + (gate - steady) * jnp.exp2(exponent)

    e = math.exp
    decay = -time_step * LOG2E
    voltage = 100.0 * x
    rev_potassium = thermal_volt * math.log(potassium_out / potassium_in)
    rev_sodium = thermal_volt * math.log(sodium_out / sodium_in)
    rev_slow = thermal_volt * math.log((potassium_out + 0.03 * sodium_out) / (potassium_in + 0.03 * sodium_in))
    up20 = power(1 / 20)
    up10 = up20 * up20
    up5 = up10 * up10
    down20 = power(-1 / 20)
    down10 = down20 * down20
    down5 = down10 * down10
    up15 = power(1 / 15)
    down6 = power(-1 / 6)
    down14 = power(-1 / 14)
    down7 = down14 * down14
    fall = jnp.exp2(jnp.minimum(x * (-50.0 * LOG2E) - 20.0 * LOG2E, 120.0))
    upper = inverse(1.0 + fall)
    lower = fall * upper

    above = voltage - rev_potassium
    cam = jnp.maximum(calcium, 0.02)
    past_calcium = voltage - 0.5 * thermal_volt * math.log(calcium_out / 0.001) + (0.5 * thermal_volt) * jnp.log(cam)
    past_sodium = voltage - rev_sodium
    inward_x = 1.0 + power(0.06, -0.06 * (rev_potassium + 200.0))
    inward_y = 1.0 + fall * e(20.0 + 0.5 * rev_potassium)
    inward_b = power(0.0002, 0.0002 * (100.0 - rev_potassium), 30.0) + up10 * (10.0 * e(-0.1 * rev_potassium - 1.0))
    inward = (5.405 * inward_y) * inverse(inward_y + inward_b * inward_x)
    plateau = 0.0146 * inverse(1.0 + power(-1 / 5.98, 25.0 / 5.98))
    pump = (2.724 * potassium_out / (potassium_out + 1.0) * sodium_in / (sodium_in + 40.0)) * inverse(
        1.0 + power(-0.1 / thermal_volt, 0.0, 0.1245) + power(-1.0 / thermal_volt, 0.0, 0.0353))
    whole = 1000.0 / ((87.5**3 + sodium_out**3) * (1.38 + calcium_out))
    back = power(-0.65 / thermal_volt, 0.0, 0.1)
    exchange = (power(0.35 / thermal_volt, 0.0, whole * sodium_in**3 * calcium_out)
                - back * (cam * (10.0 * 2.5 * 0.001 * whole * sodium_out**3))) * inverse(1.0 + back)
    pump_calcium = (0.1238 * cam) * inverse(cam + 0.5)
    calcium_sum = (0.08 * calact * calinact + 0.000592) * past_calcium
    ionic = (
        (14.838 * act * (act * act) * inact * slow + 0.00029) * past_sodium
        + calcium_sum
        + (0.294 * tract * trinact + 0.153 * rapact * rapinact + inward + plateau) * above
        + (0.392 * slowact * slowact) * (voltage - rev_slow)
        + pump
        + exchange
        + pump_calcium
    )
    new_x = x - (time_step / 100.0) * ionic
    new_calcium = calcium - (time_step * 0.05) * (calcium_sum + pump_calcium - 2.0 * exchange)

    a = up5 * e(7.0)
    b = power(1 / 200, -0.25)
    root = inverse(1.0 + power(-1 / 9.03, -56.86 / 9.03))
    rate = (((1.0 + e(-5.0)) * 10.0 * decay + a * (10.0 * decay)) + down5 * (e(-12.0) * 10.0 * decay)) * (1.0 + b) * inverse(2.0 + a + b)
    new_act = moved(act, root * root, rate)

    root = inverse(1.0 + power(1 / 7.43, 71.55 / 7.43))
    steady = root * root
    rate = lower * (power(-1 / 6.8, -80.0 / 6.8, 0.057 * -decay) + power(0.079, 0.0, 2.7 * -decay) + power(0.3485, 0.0, 310000.0 * -decay)) + (
        upper * (0.77 / 0.13 * -decay)) * inverse(1.0 + power(-1 / 11.1, -10.66 / 11.1))
    new_inact = moved(inact, steady, -rate)
    rate = lower * (
        (power(0.2444, 0.0, 25428.0 * -decay) + power(-0.04391, 0.0, 6.948e-06 * -decay)) * (voltage + 37.78) * inverse(1.0 + power(0.311, 0.311 * 79.23))
        - power(-0.01052, 0.0, 0.02424 * -decay) * inverse(1.0 + power(-0.1378, -0.1378 * 40.14))
    ) - upper * power(0.057, 0.0, 0.6 * -decay) * inverse(1.0 + down10 * e(-3.2))
    new_slow = moved(slow, steady, rate)

    p = 1.0 + power(-1 / 13, -35.0 / 13)
    r = 1.0 + down20 * e(2.5)
    pq = p * (1.0 + up5 * e(1.0))
    rate = (decay * pq) * r * inverse((1.96 + 0.35 * p) * r + pq)
    new_calact = moved(calact, inverse(1.0 + power(-1 / 7.5, -8.0 / 7.5)), rate)

    a = down10 * e(1.3)
    b = up10 * e(3.0)
    den = (1.0 + e(4.3)) + a + b
    rate = (decay * den) * inverse((bell(27.0, 225.0, 1102.5) + 20.0) * den + (380.0 + 200.0 * b + 180.0 * a))
    new_calinact = moved(calinact, down7 * inverse(down7 + e(20.0 / 7)), rate)

    rate = decay * inverse(bell(40.0, 1800.0, 9.5) + 0.8)
    new_tract = moved(tract, inverse(1.0 + down6 * e(20.0 / 6)), rate)

    t = 1.0 + up5 * e(-4.0)
    rate = (decay * t) * inverse((bell(45.0, 320.0, 85.0) + 3.0) * t + 5.0)
    new_trinact = moved(trinact, inverse(1.0 + up5 * e(4.0)), rate)

    rate = (decay / 2700.0 + down10 * (e(-4.5) * decay / 2700.0)) * (1.0 + power(1 / 11.5, 30.0 / 11.5))
    new_rapact = moved(rapact, inverse(1.0 + down7 * e(-26.0 / 7)), rate)

    rate = (1.0 + e(-6.0)) * decay / 3.36 + (up20 + down20) * (e(-3.0) * decay / 3.36)
    new_rapinact = moved(rapinact, inverse(1.0 + power(1 / 24, 88.0 / 24)), rate)

    y = 1.0 + up15 * e(-35.0 / 15)
    rate = (decay * y) * inverse(1400.0 * lax.rsqrt(1.0 + down6 * e(5.0 / 6)) + 80.0 * y)
    new_slowact = moved(slowact, inverse(1.0 + down14 * e(-5.0 / 14)), rate)
    return (new_x, new_act, new_inact, new_slow, new_calact, new_calinact, new_tract, new_trinact, new_rapact, new_rapinact, new_slowact, new_calcium)


def layer_tensor(layer_index, fibre):
    angle_in = fibre[0]
    angle_out = fibre[1]
    fibre_x = jnp.cos(angle_in) * jnp.cos(angle_out)
    fibre_y = jnp.sin(angle_in) * jnp.cos(angle_out)
    fibre_z = jnp.sin(angle_out)
    spread = longitudinal - transverse
    tensor_table = jnp.stack(
        [
            transverse + spread * fibre_x * fibre_x,
            transverse + spread * fibre_y * fibre_y,
            transverse + spread * fibre_z * fibre_z,
            spread * fibre_x * fibre_y,
            spread * fibre_x * fibre_z,
            spread * fibre_y * fibre_z,
        ]
    )
    layer_ids = jnp.arange(fibre.shape[1], dtype=jnp.int32)
    chosen = layer_index[:, None] == layer_ids[None, :]
    return jnp.sum(jnp.where(chosen[None], tensor_table[:, None, :], jnp.float32(0.0)), axis=2)


def level_weights(tensor, lanes):
    between = (tensor[:, 1:] + tensor[:, :-1]) / 2.0
    upward = jnp.pad(between, ((0, 0), (0, 1)))
    downward = jnp.pad(between, ((0, 0), (1, 0)))
    rows = jnp.stack(
        [
            tensor[0],
            tensor[1],
            tensor[3] / 2.0,
            upward[2],
            upward[4] / 2.0,
            upward[5] / 2.0,
            downward[2],
            downward[4] / 2.0,
            downward[5] / 2.0,
        ]
    )
    return jnp.broadcast_to(rows[:, :, None], rows.shape + (lanes,))


def edge_kernel(state_ref, mask_ref, edge_ref):
    depth, width = state_ref.shape[2], state_ref.shape[3]
    cells = state_ref.shape[1]
    lane = lax.broadcasted_iota(jnp.int32, (depth, LANES), 1)

    def packed(first, last):
        total = jnp.zeros((depth, LANES), jnp.float32)
        for i in range(cells):
            joined = jnp.where(lane < EDGE, first(i), last(i))
            turned = pltpu.roll(joined, i * GROUP + EDGE, 1)
            total = jnp.where(lane // GROUP == i, turned, total)
        return total

    def some(k, carry):
        for q in range(3):
            c = 3 * k + q
            edge_ref[c] = packed(
                lambda i: state_ref[c, i, :, :LANES], lambda i: state_ref[c, i, :, width - LANES :]
            )
        return carry

    lax.fori_loop(0, COMPS // 3, some, 0)
    spread = lambda i, b: jnp.broadcast_to(mask_ref[:, 2 * i + b : 2 * i + b + 1], (depth, LANES))
    edge_ref[COMPS] = packed(lambda i: spread(i, 0), lambda i: spread(i, 1))


def react_tile(store, held, place, level, part):
    rows = pl.ds(level * 8, 8)
    live = held[place, rows, part]
    new = react([store[c, place, rows, part] for c in range(COMPS)])
    for c in range(1, COMPS):
        pltpu.store(store.at[c, place, rows, part], new[c], mask=live > 0.5)
    return live, new[0]


def react_rows(main, inside, pot, rows):
    for x in rows:
        for level in range(main.shape[2] // 8):
            for i in range(main.shape[3] // LANES):
                part = pl.ds(i * LANES, LANES)
                live, u = react_tile(main, inside, x, level, part)
                pltpu.store(main.at[0, x, pl.ds(level * 8, 8), part], u, mask=live > 0.5)
                pot[x, pl.ds(level * 8, 8), part] = live * u


def shift_row(pot, dy_ref, sy_ref, x, ext, strip_row):
    shape = (pot.shape[1], LANES)
    lane = lax.broadcasted_iota(jnp.int32, shape, 1)
    first_lane, last_lane = lane == 0, lane == LANES - 1
    block = pl.ds(pl.multiple_of(ext // 8 * LANES, LANES), LANES)
    place = lax.rem(ext, 8) * GROUP
    before = pltpu.roll(strip_row(0, block), lax.rem(2 * LANES - place - (EDGE - 1), LANES), 1)
    after = pltpu.roll(strip_row(1, block), lax.rem(2 * LANES - 1 - place - EDGE, LANES), 1)
    near, far = pot[x, :, :LANES], pot[x, :, LANES:]
    near_up, far_up = pltpu.roll(near, 1, 1), pltpu.roll(far, 1, 1)
    near_down, far_down = pltpu.roll(near, LANES - 1, 1), pltpu.roll(far, LANES - 1, 1)
    lower = jnp.where(first_lane, before, near_up)
    upper = jnp.where(last_lane, far_down, near_down)
    dy_ref[x, :, :LANES] = upper - lower
    sy_ref[x, :, :LANES] = upper + lower
    lower = jnp.where(first_lane, near_up, far_up)
    upper = jnp.where(last_lane, after, far_down)
    dy_ref[x, :, LANES:] = upper - lower
    sy_ref[x, :, LANES:] = upper + lower


def spread(weight_ref, p, dx, sx, dy, sy, cross):
    depth, lanes = p.shape
    w = [weight_ref[i, :, :lanes] for i in range(9)]
    rising = w[3] * p - w[4] * dx - w[5] * dy
    falling = w[6] * p + w[7] * dx + w[8] * dy
    return (
        w[0] * sx
        + w[1] * sy
        + w[2] * cross
        + pltpu.roll(rising, 1, 0)
        + pltpu.roll(falling, depth - 1, 0)
    )


def row_spread(weight_ref, pot, dy_ref, sy_ref, x):
    before, after = pot[x - 1], pot[x + 1]
    return spread(
        weight_ref,
        pot[x],
        after - before,
        after + before,
        dy_ref[x],
        sy_ref[x],
        dy_ref[x + 1] - dy_ref[x - 1],
    )


def strip_spread(weight_ref, p):
    long = p.shape[1]
    lower, upper = pltpu.roll(p, 1, 1), pltpu.roll(p, long - 1, 1)
    before, after = pltpu.roll(p, GROUP, 1), pltpu.roll(p, long - GROUP, 1)
    dy = upper - lower
    cross = pltpu.roll(dy, long - GROUP, 1) - pltpu.roll(dy, GROUP, 1)
    return spread(weight_ref, p, after - before, after + before, dy, upper + lower, cross)


def near_kernel(
    left_hbm,
    state_hbm,
    right_hbm,
    strip_left_ref,
    strip_ref,
    strip_right_ref,
    weight_ref,
    main_out,
    inside,
    total,
    strip_track,
    track,
    main,
    pot,
    dy_ref,
    sy_ref,
    strip,
    strip_inside,
    strip_total,
    sems,
    out_sems,
):
    cells, depth, width = state_hbm.shape[1:]
    near = left_hbm.shape[1]
    span = 3 * cells
    skip = cells - near
    count = cells + 2 * near
    sides = (0, 1)
    copies = [
        pltpu.make_async_copy(source, main.at[:, pl.ds(start, source.shape[1])], sems.at[i])
        for i, (start, source) in enumerate(
            ((0, left_hbm), (near, state_hbm), (near + cells, right_hbm))
        )
    ]
    for copy in copies:
        copy.start()

    for i, source in enumerate((strip_left_ref, strip_ref, strip_right_ref)):
        part = pl.ds(i * LANES, LANES)
        for side in sides:
            for c in range(COMPS):
                strip[c, side, :, part] = source[side * (COMPS + 1) + c]
            strip_inside[side, :, part] = source[side * (COMPS + 1) + COMPS]
        codes = source[2 * (COMPS + 1)]
        for x in range(cells):
            for b in range(width // LANES):
                value = jnp.broadcast_to(codes[:, 2 * x + b : 2 * x + b + 1], (depth, LANES))
                inside[i * cells + x, :, b * LANES : (b + 1) * LANES] = value

    def shift_mask(k, carry):
        for q in range(4):
            x = 4 * k + q
            shift_row(inside, dy_ref, sy_ref, x, x, lambda side, block: strip_inside[side, :, block])
        return carry

    lax.fori_loop(0, span // 4, shift_mask, 0)

    def total_rows(k, carry):
        for q in range(2):
            x = 1 + 2 * k + q
            total[x] = row_spread(weight_ref, inside, dy_ref, sy_ref, x)
        return carry

    lax.fori_loop(0, span // 2 - 1, total_rows, 0)
    for side in sides:
        strip_total[side] = strip_spread(weight_ref, strip_inside[side])
    for copy in copies:
        copy.wait()

    def finished(s, wait):
        for q, row in enumerate((s, count - 1 - s)):
            copy = pltpu.make_async_copy(
                main.at[:, pl.ds(row, 1)], main_out.at[:, pl.ds(row, 1)], out_sems.at[2 * s + q]
            )
            if wait:
                copy.wait()
            else:
                copy.start()

    def step(s, carry):
        for side in sides:
            for level in range(depth // 8):
                for i in range(3):
                    part = pl.ds(i * LANES, LANES)
                    rows = pl.ds(level * 8, 8)
                    live, u = react_tile(strip, strip_inside, side, level, part)
                    pltpu.store(strip.at[0, side, rows, part], u, mask=live > 0.5)
                    strip_track[s, side, rows, part] = live * u

        def react_some(k, carry):
            react_rows(main, inside.at[pl.ds(skip, count)], pot, (s + 2 * k, s + 2 * k + 1))
            return carry

        lax.fori_loop(0, count // 2 - s, react_some, 0)

        def shift_some(k, carry):
            for q in range(4):
                x = 4 * k + q
                shift_row(
                    pot, dy_ref, sy_ref, x, skip + x, lambda side, block: strip_track[s, side, :, block]
                )
            return carry

        lax.fori_loop(0, count // 4, shift_some, 0)
        for q, row in enumerate((s + 1, count - 2 - s)):
            track[s, q, 0] = pot[row]
            track[s, q, 1] = dy_ref[row]

        def diffuse_some(k, carry):
            for q in range(2):
                x = s + 1 + 2 * k + q
                u = main[0, x]
                flow = row_spread(weight_ref, pot, dy_ref, sy_ref, x) - u * total[skip + x]
                main[0, x] = u + inside[skip + x] * flow
            return carry

        lax.fori_loop(0, count // 2 - 1 - s, diffuse_some, 0)
        for side in sides:
            u = strip[0, side]
            flow = strip_spread(weight_ref, strip_track[s, side]) - u * strip_total[side]
            strip[0, side] = u + strip_inside[side] * flow
        finished(s, False)
        return carry

    lax.fori_loop(0, STEPS, step, 0)
    lax.fori_loop(0, STEPS, lambda s, carry: finished(s, True) or carry, 0)


def far_kernel(
    left_hbm,
    main_hbm,
    right_hbm,
    inside,
    total,
    strip_track,
    track,
    weight_ref,
    out_hbm,
    main,
    pot,
    dy_ref,
    sy_ref,
    sems,
):
    cells, depth, width = out_hbm.shape[1:]
    far = left_hbm.shape[1]
    count = main_hbm.shape[1]
    span = far + count + far
    copies = [
        pltpu.make_async_copy(source, main.at[:, pl.ds(start, source.shape[1])], sems.at[i])
        for i, (start, source) in enumerate(
            ((0, left_hbm), (far, main_hbm), (far + count, right_hbm))
        )
    ]
    for copy in copies:
        copy.start()
    for copy in copies:
        copy.wait()

    def step(s, carry):
        starts = (s, span - far - s)

        def react_some(k, carry):
            row = jnp.where(k < far // 2, s + 2 * k, span - 2 * far - s + 2 * k)
            react_rows(main, inside, pot, (row, row + 1))
            return carry

        lax.fori_loop(0, far, react_some, 0)
        for q, row in enumerate((s + far, span - 1 - far - s)):
            pot[row] = inside[row] * main[0, row]
        for first in (s, span - 1 - far - s):
            for q in range(far + 1):
                x = first + q
                shift_row(
                    pot, dy_ref, sy_ref, x, x, lambda side, block: strip_track[s, side, :, block]
                )
        for q, row in enumerate((s + far + 1, span - 2 - far - s)):
            pot[row] = track[s, q, 0]
            dy_ref[row] = track[s, q, 1]
        for first in (s + 1, span - 1 - far - s):
            for q in range(far):
                x = first + q
                u = main[0, x]
                flow = row_spread(weight_ref, pot, dy_ref, sy_ref, x) - u * total[x]
                main[0, x] = u + inside[x] * flow
        return carry

    lax.fori_loop(0, STEPS, step, 0)
    copy = pltpu.make_async_copy(main.at[:, pl.ds(cells, cells)], out_hbm, sems.at[0])
    copy.start()
    copy.wait()


def shards(state, tissue_mask, layer_index, fibre):
    comps, cells, depth, width = state.shape
    across, along = lax.axis_size("gx"), lax.axis_size("gy")
    half = cells // 2
    span = 3 * cells
    f32 = jnp.float32

    def passed(upward, downward, axis, size):
        up = [(i, i + 1) for i in range(size - 1)]
        down = [(j, i) for i, j in up]
        return lax.ppermute(upward, axis, up), lax.ppermute(downward, axis, down)

    vmem = pl.BlockSpec(memory_space=pltpu.VMEM)
    hbm = pl.BlockSpec(memory_space=pl.ANY)
    params = pltpu.CompilerParams(vmem_limit_bytes=40 << 20)
    low, high = state[:, :half], state[:, half:]
    near_left, near_right = passed(high, low, "gx", across)

    blocks = tissue_mask.shape[2]
    codes = (tissue_mask > 0).astype(f32).transpose(1, 0, 2).reshape(depth, cells * blocks)
    codes = jnp.pad(codes, ((0, 0), (0, LANES - cells * blocks)))
    edge = pl.pallas_call(
        edge_kernel,
        out_shape=jax.ShapeDtypeStruct((comps + 1, depth, LANES), f32),
        in_specs=[vmem, vmem],
        out_specs=vmem,
        compiler_params=params,
        name="edges",
    )(state, codes)
    edge_before, edge_after = passed(edge, edge, "gy", along)
    outer = lax.broadcasted_iota(jnp.int32, edge.shape, 2) % GROUP < EDGE
    strips = jnp.concatenate(
        [jnp.where(outer, edge_before, edge), jnp.where(outer, edge, edge_after), codes[None]]
    )
    strips_left, strips_right = passed(strips, strips, "gx", across)
    low, high, strips = lax.optimization_barrier((low, high, strips))
    far_left, far_right = passed(low, high, "gx", across)

    weights = level_weights(layer_tensor(layer_index, fibre), 3 * LANES)
    count = cells + 2 * half
    row_cost = comps * depth * width * 60
    main, inside, total, strip_track, track = pl.pallas_call(
        near_kernel,
        out_shape=[
            jax.ShapeDtypeStruct((comps, count, depth, width), f32),
            jax.ShapeDtypeStruct((span, depth, width), f32),
            jax.ShapeDtypeStruct((span, depth, width), f32),
            jax.ShapeDtypeStruct((STEPS, 2, depth, 3 * LANES), f32),
            jax.ShapeDtypeStruct((STEPS, 2, 2, depth, width), f32),
        ],
        in_specs=[hbm, hbm, hbm, vmem, vmem, vmem, vmem],
        out_specs=[hbm, vmem, vmem, vmem, vmem],
        scratch_shapes=[
            pltpu.VMEM((comps, count, depth, width), f32),
            pltpu.VMEM((count, depth, width), f32),
            pltpu.VMEM((span, depth, width), f32),
            pltpu.VMEM((span, depth, width), f32),
            pltpu.VMEM((comps, 2, depth, 3 * LANES), f32),
            pltpu.VMEM((2, depth, 3 * LANES), f32),
            pltpu.VMEM((2, depth, 3 * LANES), f32),
            pltpu.SemaphoreType.DMA((3,)),
            pltpu.SemaphoreType.DMA((2 * STEPS,)),
        ],
        compiler_params=params,
        cost_estimate=pl.CostEstimate(flops=96 * row_cost, bytes_accessed=8 << 20, transcendentals=0),
        name="near",
    )(near_left, state, near_right, strips_left, strips, strips_right, weights)
    return pl.pallas_call(
        far_kernel,
        out_shape=jax.ShapeDtypeStruct(state.shape, state.dtype),
        in_specs=[hbm, hbm, hbm, vmem, vmem, vmem, vmem, vmem],
        out_specs=hbm,
        scratch_shapes=[
            pltpu.VMEM((comps, span, depth, width), f32),
            pltpu.VMEM((span, depth, width), f32),
            pltpu.VMEM((span, depth, width), f32),
            pltpu.VMEM((span, depth, width), f32),
            pltpu.SemaphoreType.DMA((3,)),
        ],
        compiler_params=params,
        cost_estimate=pl.CostEstimate(flops=64 * row_cost, bytes_accessed=8 << 20, transcendentals=0),
        name="far",
    )(far_left, main, far_right, inside, total, strip_track, track, weights)


def solution(mesh):
    placed = (P(None, "gx", None, "gy"), P("gx", None, "gy"), P(), P())
    return jax.shard_map(
        shards, mesh=mesh, in_specs=placed, out_specs=P(None, "gx", None, "gy"), check_vma=False
    )
```

```python
import math

import jax
import jax.numpy as jnp
from jax import lax
from jax.experimental import pallas as pl
from jax.experimental.pallas import tpu as pltpu
from jax.sharding import PartitionSpec as P


STEPS = 8
COMPS = 12
EDGE = 8
GROUP = 2 * EDGE
LANES = 128

time_step = 0.02
thermal_volt = 8314.472 * 310.0 / 96485.3415
potassium_out = 5.4
sodium_out = 140.0
calcium_out = 2.0
potassium_in = 138.3
sodium_in = 7.67
transverse = 0.04
longitudinal = 0.12
LOG2E = math.log2(math.e)


def react(state):
    (x, act, inact, slow, calact, calinact, tract, trinact, rapact, rapinact, slowact, calcium) = state

    def power(rate, offset=0.0, scale=1.0):
        shift = offset * LOG2E + math.log2(scale)
        scaled = x * (100.0 * rate * LOG2E)
        return jnp.exp2(scaled + shift if shift else scaled)

    def bell(centre, width, scale):
        root = math.sqrt(LOG2E / width)
        away = x * (100.0 * root) + centre * root
        return jnp.exp2(math.log2(scale) - away * away)

    def step(rate, offset):
        return jax.nn.sigmoid(x * (100.0 * rate) + offset)

    def inverse(value):
        return 1.0 / value

    def moved(gate, steady, exponent):
        return steady + (gate - steady) * jnp.exp2(exponent)

    e = math.exp
    speed = time_step * LOG2E
    voltage = 100.0 * x
    rev_potassium = thermal_volt * math.log(potassium_out / potassium_in)
    rev_sodium = thermal_volt * math.log(sodium_out / sodium_in)
    rev_slow = thermal_volt * math.log(
        (potassium_out + 0.03 * sodium_out) / (potassium_in + 0.03 * sodium_in)
    )
    up20 = power(1 / 20)
    up10 = up20 * up20
    up5 = up10 * up10
    down20 = power(-1 / 20)
    down10 = down20 * down20
    down5 = down10 * down10
    up15 = power(1 / 15)
    down6 = power(-1 / 6)
    down14 = power(-1 / 14)
    down7 = down14 * down14
    fall = jnp.exp2(jnp.minimum(x * (-50.0 * LOG2E) - 20.0 * LOG2E, 120.0))
    minus_upper = inverse(-1.0 - fall)
    minus_lower = fall * minus_upper

    above = voltage - rev_potassium
    cam = jnp.maximum(calcium, 0.02)
    past_calcium = (voltage - 0.5 * thermal_volt * math.log(calcium_out / 0.001)) + (
        0.5 * thermal_volt
    ) * jnp.log(cam)
    past_sodium = voltage - rev_sodium
    inward_x = 1.0 + power(0.06, -0.06 * (rev_potassium + 200.0))
    inward_y = 1.0 + fall * e(20.0 + 0.5 * rev_potassium)
    inward_b = power(0.0002, 0.0002 * (100.0 - rev_potassium), 30.0) + up10 * (
        10.0 * e(-0.1 * rev_potassium - 1.0)
    )
    inward = (5.405 * inward_y) * inverse(inward_y + inward_b * inward_x)
    plateau = inverse(1.0 / 0.0146 + power(-1 / 5.98, 25.0 / 5.98, 1.0 / 0.0146))
    full = power(-1.0 / thermal_volt)
    pump_top = 2.724 * potassium_out / (potassium_out + 1.0) * sodium_in / (sodium_in + 40.0)
    pump = inverse(
        (power(-0.1 / thermal_volt, 0.0, 0.1245 / pump_top) + 1.0 / pump_top)
        + full * (0.0353 / pump_top)
    )
    whole = 1000.0 / ((87.5**3 + sodium_out**3) * (1.38 + calcium_out))
    inner = whole * sodium_in**3 * calcium_out
    exchange = (inner - (cam * (2.5 * 0.001 * whole * sodium_out**3)) * full) * inverse(
        power(-0.35 / thermal_volt) + 0.1 * full
    )
    pump_calcium = 0.1238 - 0.0619 * inverse(cam + 0.5)
    calcium_sum = (0.08 * calact * calinact + 0.000592) * past_calcium + pump_calcium
    ionic = (
        (14.838 * act * (act * act) * inact * slow + 0.00029) * past_sodium
        + calcium_sum
        + (0.294 * tract * trinact + 0.153 * rapact * rapinact + inward + plateau) * above
        + (0.392 * slowact * slowact) * (voltage - rev_slow)
        + pump
        + exchange
    )
    new_x = x - (time_step / 100.0) * ionic
    new_calcium = calcium - (time_step * 0.05) * (calcium_sum - 2.0 * exchange)

    a = up5 * (e(7.0))
    b = power(1 / 200, -0.25)
    root = step(1 / 9.03, 56.86 / 9.03)
    rate = ((a * (-10.0 * speed) - (1.0 + e(-5.0)) * 10.0 * speed) - down5 * (e(-12.0) * 10.0 * speed)) * (
        (1.0 + b) * inverse(2.0 + a + b)
    )
    new_act = moved(act, root * root, rate)

    root = step(-1 / 7.43, -71.55 / 7.43)
    steady = root * root
    rate = minus_lower * (
        power(-1 / 6.8, -80.0 / 6.8, 0.057 * speed)
        + power(0.079, 0.0, 2.7 * speed)
        + power(0.3485, 0.0, 310000.0 * speed)
    ) + minus_upper * inverse(
        1.0 / (0.77 / 0.13 * speed) + power(-1 / 11.1, -10.66 / 11.1, 1.0 / (0.77 / 0.13 * speed))
    )
    new_inact = moved(inact, steady, rate)
    rate = minus_lower * (
        power(-0.01052, 0.0, 0.02424 * speed) * step(0.1378, 0.1378 * 40.14)
        - (power(0.2444, 0.0, 25428.0 * speed) + power(-0.04391, 0.0, 6.948e-06 * speed))
        * ((voltage + 37.78) * step(-0.311, -0.311 * 79.23))
    ) + minus_upper * (
        power(0.057) * inverse(1.0 / (0.6 * speed) + down10 * (e(-3.2) / (0.6 * speed)))
    )
    new_slow = moved(slow, steady, rate)

    p = 1.0 + power(-1 / 13, -35.0 / 13)
    r = down20 * (-speed * e(2.5)) - speed
    pq = p * (1.0 + up5 * e(1.0))
    rate = pq * (r * inverse((-1.96 / speed - (0.35 / speed) * p) * r + pq))
    new_calact = moved(calact, step(1 / 7.5, 8.0 / 7.5), rate)

    b = up10 * (-speed * e(3.0))
    den = (down10 * (-speed * e(1.3)) - speed * (1.0 + e(4.3))) + b
    rate = den * inverse(
        (380.0 - 180.0 * (1.0 + e(4.3)) - (20.0 / speed) * b)
        - (bell(27.0, 225.0, 1102.5 / speed) + 200.0 / speed) * den
    )
    new_calinact = moved(calinact, down7 * inverse(down7 + e(20.0 / 7)), rate)

    rate = inverse(-0.8 / speed - bell(40.0, 1800.0, 9.5 / speed))
    new_tract = moved(tract, inverse(1.0 + down6 * e(20.0 / 6)), rate)

    t = up5 * (-speed * e(-4.0)) - speed
    rate = t * inverse(5.0 - (bell(45.0, 320.0, 85.0 / speed) + 3.0 / speed) * t)
    new_trinact = moved(trinact, inverse(1.0 + up5 * e(4.0)), rate)

    rate = (down10 * (-speed * e(-4.5) / 2700.0) - speed / 2700.0) * (
        1.0 + power(1 / 11.5, 30.0 / 11.5)
    )
    new_rapact = moved(rapact, inverse(1.0 + down7 * e(-26.0 / 7)), rate)

    rate = (up20 + down20) * (-speed * e(-3.0) / 3.36) - speed * (1.0 + e(-6.0)) / 3.36
    new_rapinact = moved(rapinact, step(-1 / 24, -88.0 / 24), rate)

    y = up15 * (-speed * e(-35.0 / 15)) - speed
    rate = y * inverse(
        lax.rsqrt(1.0 / 1400.0**2 + down6 * (e(5.0 / 6) / 1400.0**2)) - (80.0 / speed) * y
    )
    new_slowact = moved(slowact, inverse(1.0 + down14 * e(-5.0 / 14)), rate)
    return (
        new_x,
        new_act,
        new_inact,
        new_slow,
        new_calact,
        new_calinact,
        new_tract,
        new_trinact,
        new_rapact,
        new_rapinact,
        new_slowact,
        new_calcium,
    )


def layer_tensor(layer_index, fibre):
    angle_in = fibre[0]
    angle_out = fibre[1]
    fibre_x = jnp.cos(angle_in) * jnp.cos(angle_out)
    fibre_y = jnp.sin(angle_in) * jnp.cos(angle_out)
    fibre_z = jnp.sin(angle_out)
    spread = longitudinal - transverse
    tensor_table = jnp.stack(
        [
            transverse + spread * fibre_x * fibre_x,
            transverse + spread * fibre_y * fibre_y,
            transverse + spread * fibre_z * fibre_z,
            spread * fibre_x * fibre_y,
            spread * fibre_x * fibre_z,
            spread * fibre_y * fibre_z,
        ]
    )
    layer_ids = jnp.arange(fibre.shape[1], dtype=jnp.int32)
    chosen = layer_index[:, None] == layer_ids[None, :]
    return jnp.sum(jnp.where(chosen[None], tensor_table[:, None, :], jnp.float32(0.0)), axis=2)


def level_weights(tensor, lanes):
    between = (tensor[:, 1:] + tensor[:, :-1]) / 2.0
    upward = jnp.pad(between, ((0, 0), (0, 1)))
    downward = jnp.pad(between, ((0, 0), (1, 0)))
    rows = jnp.stack(
        [
            tensor[0],
            tensor[1],
            tensor[3] / 2.0,
            upward[2],
            upward[4] / 2.0,
            upward[5] / 2.0,
            downward[2],
            downward[4] / 2.0,
            downward[5] / 2.0,
        ]
    )
    return jnp.broadcast_to(rows[:, :, None], rows.shape + (lanes,))


def first_kernel(state_hbm, mask_ref, inner_hbm, outer_hbm, edge_ref, main, inside, sems):
    cells, depth, width = state_hbm.shape[1:]
    half = cells // 2
    odd = lax.rem(lax.axis_index("gx"), 2)
    copies = [
        pltpu.make_async_copy(state_hbm.at[:, pl.ds(2 * i, 2)], main.at[:, pl.ds(2 * i, 2)], sems.at[i])
        for i in range(cells // 2)
    ]
    for copy in copies:
        copy.start()
    for x in range(cells):
        for b in range(width // LANES):
            part = pl.ds(b * LANES, LANES)
            code = mask_ref[:, 2 * x + b : 2 * x + b + 1]
            inside[x, :, part] = jnp.broadcast_to(code, (depth, LANES))
    for i, copy in enumerate(copies):
        copy.wait()
        react_rows(main, inside, None, (2 * i, 2 * i + 1))
    copies = [
        pltpu.make_async_copy(main.at[:, pl.ds((1 - odd) * half, half)], inner_hbm, sems.at[0]),
        pltpu.make_async_copy(main.at[:, pl.ds(odd * half, half)], outer_hbm, sems.at[1]),
    ]
    for copy in copies:
        copy.start()
    lane = lax.broadcasted_iota(jnp.int32, (depth, LANES), 1)

    def packed(first, last):
        total = jnp.zeros((depth, LANES), jnp.float32)
        for i in range(cells):
            joined = jnp.where(lane < EDGE, first(i), last(i))
            turned = pltpu.roll(joined, i * GROUP + EDGE, 1)
            total = jnp.where(lane // GROUP == i, turned, total)
        return total

    def some(k, carry):
        for q in range(3):
            c = 3 * k + q
            edge_ref[c] = packed(
                lambda i: main[c, i, :, :LANES], lambda i: main[c, i, :, width - LANES :]
            )
        return carry

    lax.fori_loop(0, COMPS // 3, some, 0)
    edge_ref[COMPS] = packed(
        lambda i: inside[i, :, :LANES], lambda i: inside[i, :, width - LANES :]
    )
    for copy in copies:
        copy.wait()


def react_tile(store, held, place, level, part):
    rows = pl.ds(level * 8, 8)
    live = held[place, rows, part]
    new = react([store[c, place, rows, part] for c in range(COMPS)])
    for c in range(1, COMPS):
        pltpu.store(store.at[c, place, rows, part], new[c], mask=live > 0.5)
    return live, new[0]


def react_rows(main, inside, pot, rows):
    for x in rows:
        for level in range(main.shape[2] // 8):
            for i in range(main.shape[3] // LANES):
                part = pl.ds(i * LANES, LANES)
                live, u = react_tile(main, inside, x, level, part)
                pltpu.store(main.at[0, x, pl.ds(level * 8, 8), part], u, mask=live > 0.5)
                if pot is not None:
                    pot[x, pl.ds(level * 8, 8), part] = live * u


def shift_row(pot, dy_ref, sy_ref, x, ext, strip_row):
    shape = (pot.shape[1], LANES)
    lane = lax.broadcasted_iota(jnp.int32, shape, 1)
    first_lane, last_lane = lane == 0, lane == LANES - 1
    block = pl.ds(pl.multiple_of(ext // 8 * LANES, LANES), LANES)
    place = lax.rem(ext, 8) * GROUP
    before = pltpu.roll(strip_row(0, block), lax.rem(2 * LANES - place - (EDGE - 1), LANES), 1)
    after = pltpu.roll(strip_row(1, block), lax.rem(2 * LANES - 1 - place - EDGE, LANES), 1)
    near, far = pot[x, :, :LANES], pot[x, :, LANES:]
    near_up, far_up = pltpu.roll(near, 1, 1), pltpu.roll(far, 1, 1)
    near_down, far_down = pltpu.roll(near, LANES - 1, 1), pltpu.roll(far, LANES - 1, 1)
    lower = jnp.where(first_lane, before, near_up)
    upper = jnp.where(last_lane, far_down, near_down)
    dy_ref[x, :, :LANES] = upper - lower
    sy_ref[x, :, :LANES] = upper + lower
    lower = jnp.where(first_lane, near_up, far_up)
    upper = jnp.where(last_lane, after, far_down)
    dy_ref[x, :, LANES:] = upper - lower
    sy_ref[x, :, LANES:] = upper + lower


def spread(weight_ref, p, dx, sx, dy, sy, cross):
    depth, lanes = p.shape
    w = [weight_ref[i, :, :lanes] for i in range(9)]
    rising = w[3] * p - w[4] * dx - w[5] * dy
    falling = w[6] * p + w[7] * dx + w[8] * dy
    return (
        w[0] * sx
        + w[1] * sy
        + w[2] * cross
        + pltpu.roll(rising, 1, 0)
        + pltpu.roll(falling, depth - 1, 0)
    )


def row_spread(weight_ref, pot, dy_ref, sy_ref, x):
    before, after = pot[x - 1], pot[x + 1]
    return spread(
        weight_ref,
        pot[x],
        after - before,
        after + before,
        dy_ref[x],
        sy_ref[x],
        dy_ref[x + 1] - dy_ref[x - 1],
    )


def strip_spread(weight_ref, p):
    long = p.shape[1]
    lower, upper = pltpu.roll(p, 1, 1), pltpu.roll(p, long - 1, 1)
    before, after = pltpu.roll(p, GROUP, 1), pltpu.roll(p, long - GROUP, 1)
    dy = upper - lower
    cross = pltpu.roll(dy, long - GROUP, 1) - pltpu.roll(dy, GROUP, 1)
    return spread(weight_ref, p, after - before, after + before, dy, upper + lower, cross)


def near_kernel(
    inner_hbm,
    facing_inner_hbm,
    facing_outer_hbm,
    outer_hbm,
    strip_inner_ref,
    strip_ref,
    strip_outer_ref,
    weight_ref,
    main_out,
    inside,
    total,
    strip_track,
    track,
    main,
    pot,
    dy_ref,
    sy_ref,
    strip,
    strip_inside,
    strip_total,
    sems,
    out_sems,
):
    near, depth, width = inner_hbm.shape[1:]
    cells = 2 * near
    odd = lax.rem(lax.axis_index("gx"), 2)
    span = 3 * cells
    skip = cells - near
    count = cells + 2 * near
    sides = (0, 1)
    copies = [
        pltpu.make_async_copy(source, main.at[:, pl.ds(start, source.shape[1])], sems.at[i])
        for i, (start, source) in enumerate(
            (
                (3 * near - 3 * near * odd, inner_hbm),
                (2 * near - near * odd, facing_inner_hbm),
                (near + near * odd, facing_outer_hbm),
                (3 * near * odd, outer_hbm),
            )
        )
    ]
    for copy in copies:
        copy.start()

    for i, source in (
        (2 - 2 * odd, strip_inner_ref),
        (1, strip_ref),
        (2 * odd, strip_outer_ref),
    ):
        part = pl.ds(pl.multiple_of(i * LANES, LANES), LANES)
        for side in sides:
            for c in range(COMPS):
                strip[c, side, :, part] = source[side * (COMPS + 1) + c]
            strip_inside[side, :, part] = source[side * (COMPS + 1) + COMPS]
        codes = source[2 * (COMPS + 1)]
        for x in range(cells):
            for b in range(width // LANES):
                value = jnp.broadcast_to(codes[:, 2 * x + b : 2 * x + b + 1], (depth, LANES))
                inside[i * cells + x, :, b * LANES : (b + 1) * LANES] = value

    def shift_mask(k, carry):
        for q in range(4):
            x = 4 * k + q
            shift_row(inside, dy_ref, sy_ref, x, x, lambda side, block: strip_inside[side, :, block])
        return carry

    lax.fori_loop(0, span // 4, shift_mask, 0)

    def total_rows(k, carry):
        for q in range(2):
            x = 1 + 2 * k + q
            total[x] = row_spread(weight_ref, inside, dy_ref, sy_ref, x)
        return carry

    lax.fori_loop(0, span // 2 - 1, total_rows, 0)
    for side in sides:
        strip_total[side] = strip_spread(weight_ref, strip_inside[side])
    for copy in copies:
        copy.wait()

    def finished(s, wait):
        for q, row in enumerate((s, count - 1 - s)):
            copy = pltpu.make_async_copy(
                main.at[:, pl.ds(row, 1)], main_out.at[:, pl.ds(row, 1)], out_sems.at[2 * s + q]
            )
            if wait:
                copy.wait()
            else:
                copy.start()

    def start_row(x, carry):
        pot[x] = inside[skip + x] * main[0, x]
        return carry

    lax.fori_loop(0, count, start_row, 0)
    for side in sides:
        strip_track[0, side] = strip_inside[side] * strip[0, side]

    def step(s, carry):
        def shift_some(k, carry):
            for q in range(4):
                x = 4 * k + q
                shift_row(
                    pot, dy_ref, sy_ref, x, skip + x, lambda side, block: strip_track[s, side, :, block]
                )
            return carry

        lax.fori_loop(0, count // 4, shift_some, 0)
        for q, row in enumerate((s + 1, count - 2 - s)):
            track[s, q, 0] = pot[row]
            track[s, q, 1] = dy_ref[row]

        def diffuse_some(k, carry):
            for q in range(2):
                x = s + 1 + 2 * k + q
                u = main[0, x]
                flow = row_spread(weight_ref, pot, dy_ref, sy_ref, x) - u * total[skip + x]
                main[0, x] = u + inside[skip + x] * flow
            return carry

        lax.fori_loop(0, count // 2 - 1 - s, diffuse_some, 0)
        finished(s, False)

        @pl.when(s < STEPS - 1)
        def _():
            for side in sides:
                u = strip[0, side]
                flow = strip_spread(weight_ref, strip_track[s, side]) - u * strip_total[side]
                strip[0, side] = u + strip_inside[side] * flow

            def react_strip(side, carry):
                for level in range(depth // 8):
                    for i in range(3):
                        part = pl.ds(i * LANES, LANES)
                        rows = pl.ds(level * 8, 8)
                        live, u = react_tile(strip, strip_inside, side, level, part)
                        pltpu.store(strip.at[0, side, rows, part], u, mask=live > 0.5)
                        strip_track[s + 1, side, rows, part] = live * u
                return carry

            lax.fori_loop(0, 2, react_strip, 0)

            def react_some(k, carry):
                x = s + 1 + 2 * k
                react_rows(main, inside.at[pl.ds(skip, count)], pot, (x, x + 1))
                return carry

            lax.fori_loop(0, count // 2 - 1 - s, react_some, 0)

        return carry

    lax.fori_loop(0, STEPS, step, 0)
    lax.fori_loop(0, STEPS, lambda s, carry: finished(s, True) or carry, 0)


def far_kernel(
    inner_hbm,
    main_hbm,
    outer_hbm,
    inside,
    total,
    strip_track,
    track,
    weight_ref,
    out_hbm,
    main,
    pot,
    dy_ref,
    sy_ref,
    sems,
):
    cells, _, _ = out_hbm.shape[1:]
    far = inner_hbm.shape[1]
    odd = lax.rem(lax.axis_index("gx"), 2)
    count = main_hbm.shape[1]
    span = far + count + far
    copies = [
        pltpu.make_async_copy(source, main.at[:, pl.ds(start, source.shape[1])], sems.at[i])
        for i, (start, source) in enumerate(
            (
                ((1 - odd) * (far + count), inner_hbm),
                (far, main_hbm),
                (odd * (far + count), outer_hbm),
            )
        )
    ]
    for copy in copies:
        copy.start()
    for copy in copies:
        copy.wait()

    for q in range(far):
        for x in (q, span - 1 - q):
            pot[x] = inside[x] * main[0, x]

    def step(s, carry):
        for row in (s + far, span - 1 - far - s):
            pot[row] = inside[row] * main[0, row]
        for first in (s, span - 1 - far - s):
            for q in range(far + 1):
                x = first + q
                shift_row(
                    pot, dy_ref, sy_ref, x, x, lambda side, block: strip_track[s, side, :, block]
                )
        for q, row in enumerate((s + far + 1, span - 2 - far - s)):
            pot[row] = track[s, q, 0]
            dy_ref[row] = track[s, q, 1]
        for first in (s + 1, span - 1 - far - s):
            for q in range(far):
                x = first + q
                u = main[0, x]
                flow = row_spread(weight_ref, pot, dy_ref, sy_ref, x) - u * total[x]
                main[0, x] = u + inside[x] * flow

        def react_some(k, carry):
            row = jnp.where(k < far // 2, s + 1 + 2 * k, span - 2 * far - s - 1 + 2 * k)
            react_rows(main, inside, pot, (row, row + 1))
            return carry

        lax.fori_loop(0, jnp.where(s < STEPS - 1, far, 0), react_some, 0)
        return carry

    lax.fori_loop(0, STEPS, step, 0)
    copy = pltpu.make_async_copy(main.at[:, pl.ds(cells, cells)], out_hbm, sems.at[0])
    copy.start()
    copy.wait()


def shards(state, tissue_mask, layer_index, fibre):
    comps, cells, depth, width = state.shape
    across, along = lax.axis_size("gx"), lax.axis_size("gy")
    half = cells // 2
    span = 3 * cells
    f32 = jnp.float32

    def swapped(value, axis, size, first):
        pairs = [(i, i + 1) for i in range(first, size - 1, 2)]
        return lax.ppermute(value, axis, pairs + [(j, i) for i, j in pairs])

    vmem = pl.BlockSpec(memory_space=pltpu.VMEM)
    hbm = pl.BlockSpec(memory_space=pl.ANY)
    params = pltpu.CompilerParams(vmem_limit_bytes=40 << 20)
    blocks = tissue_mask.shape[2]
    codes = (tissue_mask > 0).astype(f32).transpose(1, 0, 2).reshape(depth, cells * blocks)
    codes = jnp.pad(codes, ((0, 0), (0, LANES - cells * blocks)))
    face = jax.ShapeDtypeStruct((comps, half, depth, width), f32)
    facing_inner, facing_outer, edge = pl.pallas_call(
        first_kernel,
        out_shape=[face, face, jax.ShapeDtypeStruct((comps + 1, depth, LANES), f32)],
        in_specs=[hbm, vmem],
        out_specs=[hbm, hbm, vmem],
        scratch_shapes=[
            pltpu.VMEM((comps, cells, depth, width), f32),
            pltpu.VMEM((cells, depth, width), f32),
            pltpu.SemaphoreType.DMA((cells // 2,)),
        ],
        compiler_params=params,
        name="first",
    )(state, codes)
    edge_outer = swapped(edge, "gy", along, 1)
    edge_inner = swapped(edge, "gy", along, 0)
    near_outer = swapped(facing_outer, "gx", across, 1)
    near_inner = swapped(facing_inner, "gx", across, 0)
    odd_along = lax.rem(lax.axis_index("gy"), 2) == 1
    edge_before = jnp.where(odd_along, edge_inner, edge_outer)
    edge_after = jnp.where(odd_along, edge_outer, edge_inner)
    outer = lax.broadcasted_iota(jnp.int32, edge.shape, 2) % GROUP < EDGE
    strips = jnp.concatenate(
        [jnp.where(outer, edge_before, edge), jnp.where(outer, edge, edge_after), codes[None]]
    )
    strip_outer = swapped(strips, "gx", across, 1)
    strip_inner = swapped(strips, "gx", across, 0)
    far_outer = swapped(facing_inner, "gx", across, 1)
    far_inner = swapped(facing_outer, "gx", across, 0)

    weights = level_weights(layer_tensor(layer_index, fibre), 3 * LANES)
    count = cells + 2 * half
    row_cost = comps * depth * width * 60
    main, inside, total, strip_track, track = pl.pallas_call(
        near_kernel,
        out_shape=[
            jax.ShapeDtypeStruct((comps, count, depth, width), f32),
            jax.ShapeDtypeStruct((span, depth, width), f32),
            jax.ShapeDtypeStruct((span, depth, width), f32),
            jax.ShapeDtypeStruct((STEPS, 2, depth, 3 * LANES), f32),
            jax.ShapeDtypeStruct((STEPS, 2, 2, depth, width), f32),
        ],
        in_specs=[hbm, hbm, hbm, hbm, vmem, vmem, vmem, vmem],
        out_specs=[hbm, vmem, vmem, vmem, vmem],
        scratch_shapes=[
            pltpu.VMEM((comps, count, depth, width), f32),
            pltpu.VMEM((count, depth, width), f32),
            pltpu.VMEM((span, depth, width), f32),
            pltpu.VMEM((span, depth, width), f32),
            pltpu.VMEM((comps, 2, depth, 3 * LANES), f32),
            pltpu.VMEM((2, depth, 3 * LANES), f32),
            pltpu.VMEM((2, depth, 3 * LANES), f32),
            pltpu.SemaphoreType.DMA((4,)),
            pltpu.SemaphoreType.DMA((2 * STEPS,)),
        ],
        compiler_params=params,
        cost_estimate=pl.CostEstimate(flops=96 * row_cost, bytes_accessed=8 << 20, transcendentals=0),
        name="near",
    )(
        near_inner,
        facing_inner,
        facing_outer,
        near_outer,
        strip_inner,
        strips,
        strip_outer,
        weights,
    )
    return pl.pallas_call(
        far_kernel,
        out_shape=jax.ShapeDtypeStruct(state.shape, state.dtype),
        in_specs=[hbm, hbm, hbm, vmem, vmem, vmem, vmem, vmem],
        out_specs=hbm,
        scratch_shapes=[
            pltpu.VMEM((comps, span, depth, width), f32),
            pltpu.VMEM((span, depth, width), f32),
            pltpu.VMEM((span, depth, width), f32),
            pltpu.VMEM((span, depth, width), f32),
            pltpu.SemaphoreType.DMA((3,)),
        ],
        compiler_params=params,
        cost_estimate=pl.CostEstimate(flops=64 * row_cost, bytes_accessed=8 << 20, transcendentals=0),
        name="far",
    )(far_inner, main, far_outer, inside, total, strip_track, track, weights)


def solution(mesh):
    placed = (P(None, "gx", None, "gy"), P("gx", None, "gy"), P(), P())

    return jax.shard_map(
        shards, mesh=mesh, in_specs=placed, out_specs=P(None, "gx", None, "gy"), check_vma=False
    )
```

```python
import functools
import math

import jax
import jax.numpy as jnp
from jax import lax
from jax.experimental import pallas as pl
from jax.experimental.pallas import tpu as pltpu
from jax.sharding import PartitionSpec as P


STEPS = 8
COMPS = 12
CHUNKS = (4, 4)
PLANE = 8
EDGE = 8
GROUP = 2 * EDGE
LANES = 128

time_step = 0.02
thermal_volt = 8314.472 * 310.0 / 96485.3415
potassium_out = 5.4
sodium_out = 140.0
calcium_out = 2.0
potassium_in = 138.3
sodium_in = 7.67
transverse = 0.04
longitudinal = 0.12
LOG2E = math.log2(math.e)


def react(state):
    (x, act, inact, slow, calact, calinact, tract, trinact, rapact, rapinact, slowact, calcium) = state

    def power(rate, offset=0.0, scale=1.0):
        shift = offset * LOG2E + math.log2(scale)
        scaled = x * (100.0 * rate * LOG2E)
        return jnp.exp2(scaled + shift if shift else scaled)

    def bell(centre, width, scale):
        root = math.sqrt(LOG2E / width)
        away = x * (100.0 * root) + centre * root
        return jnp.exp2(math.log2(scale) - away * away)

    def step(rate, offset):
        return jax.nn.sigmoid(x * (100.0 * rate) + offset)

    def inverse(value):
        return 1.0 / value

    def moved(gate, steady, exponent):
        return steady + (gate - steady) * jnp.exp2(exponent)

    e = math.exp
    speed = time_step * LOG2E
    voltage = 100.0 * x
    rev_potassium = thermal_volt * math.log(potassium_out / potassium_in)
    rev_sodium = thermal_volt * math.log(sodium_out / sodium_in)
    rev_slow = thermal_volt * math.log(
        (potassium_out + 0.03 * sodium_out) / (potassium_in + 0.03 * sodium_in)
    )
    up20 = power(1 / 20)
    up10 = up20 * up20
    up5 = up10 * up10
    down20 = power(-1 / 20)
    down10 = down20 * down20
    down5 = down10 * down10
    up15 = power(1 / 15)
    down6 = power(-1 / 6)
    down14 = power(-1 / 14)
    down7 = down14 * down14
    fall = jnp.exp2(jnp.minimum(x * (-50.0 * LOG2E) - 20.0 * LOG2E, 120.0))
    minus_upper = inverse(-1.0 - fall)
    minus_lower = fall * minus_upper

    above = voltage - rev_potassium
    cam = jnp.maximum(calcium, 0.02)
    past_calcium = (voltage - 0.5 * thermal_volt * math.log(calcium_out / 0.001)) + (
        0.5 * thermal_volt
    ) * jnp.log(cam)
    past_sodium = voltage - rev_sodium
    inward_x = 1.0 + power(0.06, -0.06 * (rev_potassium + 200.0))
    inward_y = 1.0 + fall * e(20.0 + 0.5 * rev_potassium)
    inward_b = power(0.0002, 0.0002 * (100.0 - rev_potassium), 30.0) + up10 * (
        10.0 * e(-0.1 * rev_potassium - 1.0)
    )
    inward = (5.405 * inward_y) * inverse(inward_y + inward_b * inward_x)
    plateau = inverse(1.0 / 0.0146 + power(-1 / 5.98, 25.0 / 5.98, 1.0 / 0.0146))
    full = power(-1.0 / thermal_volt)
    pump_top = 2.724 * potassium_out / (potassium_out + 1.0) * sodium_in / (sodium_in + 40.0)
    pump = inverse(
        (power(-0.1 / thermal_volt, 0.0, 0.1245 / pump_top) + 1.0 / pump_top)
        + full * (0.0353 / pump_top)
    )
    whole = 1000.0 / ((87.5**3 + sodium_out**3) * (1.38 + calcium_out))
    inner = whole * sodium_in**3 * calcium_out
    exchange = (inner - (cam * (2.5 * 0.001 * whole * sodium_out**3)) * full) * inverse(
        power(-0.35 / thermal_volt) + 0.1 * full
    )
    pump_calcium = 0.1238 - 0.0619 * inverse(cam + 0.5)
    calcium_sum = (0.08 * calact * calinact + 0.000592) * past_calcium + pump_calcium
    ionic = (
        (14.838 * act * (act * act) * inact * slow + 0.00029) * past_sodium
        + calcium_sum
        + (0.294 * tract * trinact + 0.153 * rapact * rapinact + inward + plateau) * above
        + (0.392 * slowact * slowact) * (voltage - rev_slow)
        + pump
        + exchange
    )
    new_x = x - (time_step / 100.0) * ionic
    new_calcium = calcium - (time_step * 0.05) * (calcium_sum - 2.0 * exchange)

    a = up5 * (e(7.0))
    b = power(1 / 200, -0.25)
    root = step(1 / 9.03, 56.86 / 9.03)
    rate = ((a * (-10.0 * speed) - (1.0 + e(-5.0)) * 10.0 * speed) - down5 * (e(-12.0) * 10.0 * speed)) * (
        (1.0 + b) * inverse(2.0 + a + b)
    )
    new_act = moved(act, root * root, rate)

    root = step(-1 / 7.43, -71.55 / 7.43)
    steady = root * root
    rate = minus_lower * (
        power(-1 / 6.8, -80.0 / 6.8, 0.057 * speed)
        + power(0.079, 0.0, 2.7 * speed)
        + power(0.3485, 0.0, 310000.0 * speed)
    ) + minus_upper * inverse(
        1.0 / (0.77 / 0.13 * speed) + power(-1 / 11.1, -10.66 / 11.1, 1.0 / (0.77 / 0.13 * speed))
    )
    new_inact = moved(inact, steady, rate)
    rate = minus_lower * (
        power(-0.01052, 0.0, 0.02424 * speed) * step(0.1378, 0.1378 * 40.14)
        - (power(0.2444, 0.0, 25428.0 * speed) + power(-0.04391, 0.0, 6.948e-06 * speed))
        * ((voltage + 37.78) * step(-0.311, -0.311 * 79.23))
    ) + minus_upper * (
        power(0.057) * inverse(1.0 / (0.6 * speed) + down10 * (e(-3.2) / (0.6 * speed)))
    )
    new_slow = moved(slow, steady, rate)

    p = 1.0 + power(-1 / 13, -35.0 / 13)
    r = down20 * (-speed * e(2.5)) - speed
    pq = p * (1.0 + up5 * e(1.0))
    rate = pq * (r * inverse((-1.96 / speed - (0.35 / speed) * p) * r + pq))
    new_calact = moved(calact, step(1 / 7.5, 8.0 / 7.5), rate)

    b = up10 * (-speed * e(3.0))
    den = (down10 * (-speed * e(1.3)) - speed * (1.0 + e(4.3))) + b
    rate = den * inverse(
        (380.0 - 180.0 * (1.0 + e(4.3)) - (20.0 / speed) * b)
        - (bell(27.0, 225.0, 1102.5 / speed) + 200.0 / speed) * den
    )
    new_calinact = moved(calinact, down7 * inverse(down7 + e(20.0 / 7)), rate)

    rate = inverse(-0.8 / speed - bell(40.0, 1800.0, 9.5 / speed))
    new_tract = moved(tract, inverse(1.0 + down6 * e(20.0 / 6)), rate)

    t = up5 * (-speed * e(-4.0)) - speed
    rate = t * inverse(5.0 - (bell(45.0, 320.0, 85.0 / speed) + 3.0 / speed) * t)
    new_trinact = moved(trinact, inverse(1.0 + up5 * e(4.0)), rate)

    rate = (down10 * (-speed * e(-4.5) / 2700.0) - speed / 2700.0) * (
        1.0 + power(1 / 11.5, 30.0 / 11.5)
    )
    new_rapact = moved(rapact, inverse(1.0 + down7 * e(-26.0 / 7)), rate)

    rate = (up20 + down20) * (-speed * e(-3.0) / 3.36) - speed * (1.0 + e(-6.0)) / 3.36
    new_rapinact = moved(rapinact, step(-1 / 24, -88.0 / 24), rate)

    y = up15 * (-speed * e(-35.0 / 15)) - speed
    rate = y * inverse(
        lax.rsqrt(1.0 / 1400.0**2 + down6 * (e(5.0 / 6) / 1400.0**2)) - (80.0 / speed) * y
    )
    new_slowact = moved(slowact, inverse(1.0 + down14 * e(-5.0 / 14)), rate)
    return (
        new_x,
        new_act,
        new_inact,
        new_slow,
        new_calact,
        new_calinact,
        new_tract,
        new_trinact,
        new_rapact,
        new_rapinact,
        new_slowact,
        new_calcium,
    )


def layer_tensor(layer_index, fibre):
    angle_in = fibre[0]
    angle_out = fibre[1]
    fibre_x = jnp.cos(angle_in) * jnp.cos(angle_out)
    fibre_y = jnp.sin(angle_in) * jnp.cos(angle_out)
    fibre_z = jnp.sin(angle_out)
    spread = longitudinal - transverse
    tensor_table = jnp.stack(
        [
            transverse + spread * fibre_x * fibre_x,
            transverse + spread * fibre_y * fibre_y,
            transverse + spread * fibre_z * fibre_z,
            spread * fibre_x * fibre_y,
            spread * fibre_x * fibre_z,
            spread * fibre_y * fibre_z,
        ]
    )
    layer_ids = jnp.arange(fibre.shape[1], dtype=jnp.int32)
    chosen = layer_index[:, None] == layer_ids[None, :]
    return jnp.sum(jnp.where(chosen[None], tensor_table[:, None, :], jnp.float32(0.0)), axis=2)


def level_weights(tensor, lanes):
    between = (tensor[:, 1:] + tensor[:, :-1]) / 2.0
    upward = jnp.pad(between, ((0, 0), (0, 1)))
    downward = jnp.pad(between, ((0, 0), (1, 0)))
    rows = jnp.stack(
        [
            tensor[0],
            tensor[1],
            tensor[3] / 2.0,
            upward[2],
            upward[4] / 2.0,
            upward[5] / 2.0,
            downward[2],
            downward[4] / 2.0,
            downward[5] / 2.0,
        ]
    )
    return jnp.broadcast_to(rows[:, :, None], rows.shape + (lanes,))


def first_kernel(chunks, state_ref, mask_ref, *refs):
    faces, (edge_ref, main, inside, sems) = refs[: 2 * len(chunks)], refs[2 * len(chunks) :]
    cells, depth, width = state_ref.shape[1:]
    odd = lax.rem(lax.axis_index("gx"), 2)
    lane = lax.broadcasted_iota(jnp.int32, (depth, LANES), 1)
    diagonal = lax.broadcasted_iota(jnp.int32, (depth, depth), 0) == lax.broadcasted_iota(
        jnp.int32, (depth, depth), 1
    )
    codes = jnp.zeros((depth, LANES), jnp.float32)
    for x in range(cells):
        for b in range(width // LANES):
            code = jnp.where(mask_ref[x, b : b + 1, :] > 0, jnp.float32(1.0), jnp.float32(0.0))
            code = jnp.where(diagonal, jnp.broadcast_to(code, (depth, depth)), jnp.float32(0.0))
            code = jnp.broadcast_to(jnp.sum(code, axis=1, keepdims=True), (depth, LANES))
            inside[x, :, pl.ds(b * LANES, LANES)] = code
            codes = jnp.where(lane == 2 * x + b, code, codes)
    edge_ref[COMPS + 1] = codes

    def react_pair(k, carry):
        for x in (2 * k, 2 * k + 1):
            for level in range(depth // 8):
                for i in range(width // LANES):
                    place = (x, pl.ds(level * 8, 8), pl.ds(i * LANES, LANES))
                    old = [state_ref[(c,) + place] for c in range(COMPS)]
                    live = inside[place] > 0.5
                    for c, new in enumerate(react(old)):
                        main[(c,) + place] = jnp.where(live, new, old[c])
        return carry

    lax.fori_loop(0, cells // 2, react_pair, 0)
    copies = []
    start = 0
    for i, rows in enumerate(chunks):
        above, below = cells - start - rows, start
        inner = above + odd * (below - above)
        outer = below + odd * (above - below)
        for face, row, sem in ((faces[2 * i], inner, 2 * i), (faces[2 * i + 1], outer, 2 * i + 1)):
            copies.append(pltpu.make_async_copy(main.at[:, pl.ds(row, rows)], face, sems.at[sem]))
        start += rows
    for copy in copies:
        copy.start()

    def packed(first, last):
        total = jnp.zeros((depth, LANES), jnp.float32)
        for i in range(cells):
            joined = jnp.where(lane < EDGE, first(i), last(i))
            turned = pltpu.roll(joined, i * GROUP + EDGE, 1)
            total = jnp.where(lane // GROUP == i, turned, total)
        return total

    def some(k, carry):
        for q in range(3):
            c = 3 * k + q
            edge_ref[c] = packed(
                lambda i: main[c, i, :, :LANES], lambda i: main[c, i, :, width - LANES :]
            )
        return carry

    lax.fori_loop(0, COMPS // 3, some, 0)
    edge_ref[COMPS] = packed(
        lambda i: inside[i, :, :LANES], lambda i: inside[i, :, width - LANES :]
    )
    for copy in copies:
        copy.wait()


def react_tile(at, live):
    new = react([at(c)[...] for c in range(COMPS)])
    for c in range(COMPS):
        pltpu.store(at(c), new[c], mask=live > 0.5)
    return live * new[0]


def react_rows(main, inside, pot, rows):
    for x in rows:
        for level in range(main.shape[2] // 8):
            for i in range(main.shape[3] // LANES):
                place = (x, pl.ds(level * 8, 8), pl.ds(i * LANES, LANES))
                held = react_tile(lambda c: main.at[(c,) + place], inside[place])
                if pot is not None:
                    pot[place] = held


def shift_row(pot, dy_ref, sy_ref, x, ext, strip_row):
    shape = (pot.shape[1], LANES)
    lane = lax.broadcasted_iota(jnp.int32, shape, 1)
    first_lane, last_lane = lane == 0, lane == LANES - 1
    block = pl.ds(pl.multiple_of(ext // 8 * LANES, LANES), LANES)
    place = lax.rem(ext, 8) * GROUP
    before = pltpu.roll(strip_row(0, block), lax.rem(2 * LANES - place - (EDGE - 1), LANES), 1)
    after = pltpu.roll(strip_row(1, block), lax.rem(2 * LANES - 1 - place - EDGE, LANES), 1)
    near, far = pot[x, :, :LANES], pot[x, :, LANES:]
    near_up, far_up = pltpu.roll(near, 1, 1), pltpu.roll(far, 1, 1)
    near_down, far_down = pltpu.roll(near, LANES - 1, 1), pltpu.roll(far, LANES - 1, 1)
    lower = jnp.where(first_lane, before, near_up)
    upper = jnp.where(last_lane, far_down, near_down)
    dy_ref[x, :, :LANES] = upper - lower
    sy_ref[x, :, :LANES] = upper + lower
    lower = jnp.where(first_lane, near_up, far_up)
    upper = jnp.where(last_lane, after, far_down)
    dy_ref[x, :, LANES:] = upper - lower
    sy_ref[x, :, LANES:] = upper + lower


def spread(weight_ref, p, dx, sx, dy, sy, cross):
    depth, lanes = p.shape
    w = [weight_ref[i, :, :lanes] for i in range(9)]
    rising = w[3] * p - w[4] * dx - w[5] * dy
    falling = w[6] * p + w[7] * dx + w[8] * dy
    return (
        w[0] * sx
        + w[1] * sy
        + w[2] * cross
        + pltpu.roll(rising, 1, 0)
        + pltpu.roll(falling, depth - 1, 0)
    )


def row_spread(weight_ref, pot, dy_ref, sy_ref, x):
    before, after = pot[x - 1], pot[x + 1]
    return spread(
        weight_ref,
        pot[x],
        after - before,
        after + before,
        dy_ref[x],
        sy_ref[x],
        dy_ref[x + 1] - dy_ref[x - 1],
    )


def strip_spread(weight_ref, p):
    long = p.shape[1]
    lower, upper = pltpu.roll(p, 1, 1), pltpu.roll(p, long - 1, 1)
    before, after = pltpu.roll(p, GROUP, 1), pltpu.roll(p, long - GROUP, 1)
    dy = upper - lower
    cross = pltpu.roll(dy, long - GROUP, 1) - pltpu.roll(dy, GROUP, 1)
    return spread(weight_ref, p, after - before, after + before, dy, upper + lower, cross)


def strip_kernel(
    strip_inner_hbm,
    strip_hbm,
    strip_outer_hbm,
    weight_ref,
    inside,
    total,
    strip_track,
    dy_ref,
    sy_ref,
    strip,
    code_ref,
    strip_total,
    sems,
):
    span, depth, width = inside.shape
    cells = span // 3
    odd = lax.rem(lax.axis_index("gx"), 2)
    sides = (0, 1)
    copies = []
    for q, (i, source) in enumerate(
        ((2 - 2 * odd, strip_inner_hbm), (1, strip_hbm), (2 * odd, strip_outer_hbm))
    ):
        part = pl.ds(pl.multiple_of(i * LANES, LANES), LANES)
        for side in sides:
            held = source.at[pl.ds(side * (COMPS + 1), COMPS + 1)]
            copies.append(
                pltpu.make_async_copy(held, strip.at[side, :, :, part], sems.at[3 * q + side])
            )
        copies.append(
            pltpu.make_async_copy(
                source.at[pl.ds(2 * (COMPS + 1), 1)], code_ref.at[pl.ds(i, 1)], sems.at[3 * q + 2]
            )
        )
    for copy in copies:
        copy.start()
    for copy in copies:
        copy.wait()
    for i in range(3):
        codes = code_ref[i]
        for x in range(cells):
            for b in range(width // LANES):
                value = jnp.broadcast_to(codes[:, 2 * x + b : 2 * x + b + 1], (depth, LANES))
                inside[i * cells + x, :, b * LANES : (b + 1) * LANES] = value

    def shift_mask(k, carry):
        for q in range(4):
            x = 4 * k + q
            shift_row(inside, dy_ref, sy_ref, x, x, lambda side, block: strip[side, COMPS, :, block])
        return carry

    lax.fori_loop(0, span // 4, shift_mask, 0)

    def total_rows(k, carry):
        for q in range(2):
            x = 1 + 2 * k + q
            total[x] = row_spread(weight_ref, inside, dy_ref, sy_ref, x)
        return carry

    lax.fori_loop(0, span // 2 - 1, total_rows, 0)
    for side in sides:
        strip_total[side] = strip_spread(weight_ref, strip[side, COMPS])
        strip_track[0, side] = strip[side, COMPS] * strip[side, 0]

    def step(s, carry):
        for side in sides:
            u = strip[side, 0]
            flow = strip_spread(weight_ref, strip_track[s, side]) - u * strip_total[side]
            strip[side, 0] = u + strip[side, COMPS] * flow

        for side in sides:
            for level in range(depth // 8):
                for i in range(3):
                    place = (pl.ds(level * 8, 8), pl.ds(i * LANES, LANES))
                    held = react_tile(
                        lambda c: strip.at[(side, c) + place], strip[(side, COMPS) + place]
                    )
                    strip_track[(s + 1, side) + place] = held
        return carry

    lax.fori_loop(0, STEPS - 1, step, 0)


def finished(main, main_out, sems, s, wait):
    count = main.shape[1]
    for q, row in enumerate((s, count - 1 - s)):
        copy = pltpu.make_async_copy(
            main.at[:, pl.ds(row, 1)], main_out.at[:, pl.ds(row, 1)], sems.at[2 * s + q]
        )
        if wait:
            copy.wait()
        else:
            copy.start()


def near_kernel(pieces, near, *refs):
    sources, refs = refs[: pieces + 2], refs[pieces + 2 :]
    inside, total, strip_track, weight_ref, main_out, track = refs[:6]
    main, pot, dy_ref, sy_ref, sems, out_sems = refs[6:]
    count, _, _ = pot.shape
    cells = count - 2 * near
    skip = cells - near
    odd = lax.rem(lax.axis_index("gx"), 2)
    inner_hbm, outer_hbm = sources[:2]
    places = [(near + cells - odd * (near + cells), inner_hbm), (odd * (near + cells), outer_hbm)]
    start = 0
    for source in sources[2:]:
        rows = source.shape[1]
        above, below = cells - start - rows, start
        places.append((near + above + odd * (below - above), source))
        start += rows
    copies = [
        pltpu.make_async_copy(source, main.at[:, pl.ds(row, source.shape[1])], sems.at[i])
        for i, (row, source) in enumerate(places)
    ]
    for copy in copies:
        copy.start()
    for copy in copies:
        copy.wait()

    group = 4 if count % 4 == 0 else 2

    def start_row(k, carry):
        for q in range(2):
            pot[2 * k + q] = inside[skip + 2 * k + q] * main[0, 2 * k + q]
        return carry

    lax.fori_loop(0, count // 2, start_row, 0)

    def step(s, carry):
        def shift_some(k, carry):
            for q in range(group):
                x = group * k + q
                shift_row(
                    pot, dy_ref, sy_ref, x, skip + x, lambda side, block: strip_track[s, side, :, block]
                )
            return carry

        lax.fori_loop(s // group, (count - 1 - s) // group + 1, shift_some, 0)
        for q, row in enumerate((s + 1, count - 2 - s)):
            track[s, q, 0] = pot[row]
            track[s, q, 1] = dy_ref[row]

        def diffuse_some(size, start, k, carry):
            for q in range(size):
                x = start + size * k + q
                u = main[0, x]
                flow = row_spread(weight_ref, pot, dy_ref, sy_ref, x) - u * total[skip + x]
                main[0, x] = u + inside[skip + x] * flow
            return carry

        pairs = jnp.maximum(count // 2 - 1 - s, 0)
        lax.fori_loop(0, pairs // 2, functools.partial(diffuse_some, 4, s + 1), 0)
        rest = s + 1 + pairs // 2 * 4
        lax.fori_loop(0, lax.rem(pairs, 2), functools.partial(diffuse_some, 2, rest), 0)

        @pl.when(s < min(STEPS, count // 2))
        def _():
            finished(main, main_out, out_sems, s, False)

        def react_some(k, carry):
            x = s + 1 + 2 * k
            react_rows(main, inside.at[pl.ds(skip, count)], pot, (x, x + 1))
            return carry

        lax.fori_loop(0, jnp.where(s < STEPS - 1, count // 2 - 1 - s, 0), react_some, 0)
        return carry

    lax.fori_loop(0, STEPS, step, 0)

    def drained(s, carry):
        finished(main, main_out, out_sems, s, True)
        return carry

    lax.fori_loop(0, min(STEPS, count // 2), drained, 0)


def ring_kernel(last, *refs):
    inner_hbm, main_hbm, outer_hbm, relay_hbm = refs[:4]
    inside, total, strip_track, track, weight_ref = refs[4:9]
    if last:
        out_hbm, main, pot, dy_ref, sy_ref, sems = refs[9:]
    else:
        main_out, track_out, main, pot, dy_ref, sy_ref, sems, out_sems = refs[9:]
    far, _, _ = inner_hbm.shape[1:]
    count = main_hbm.shape[1]
    span = far + count + far
    cells = inside.shape[0] // 3
    skip = (inside.shape[0] - span) // 2
    before = (count - cells) // 2
    odd = lax.rem(lax.axis_index("gx"), 2)
    across = lax.rem(lax.axis_index("gx") + 1, PLANE)
    relayed = jnp.logical_or(across == 0, across == 1)
    inner_place, outer_place = far + count - odd * (far + count), odd * (far + count)
    copies = [
        pltpu.make_async_copy(source, main.at[:, pl.ds(row, source.shape[1])], sems.at[i])
        for i, (row, source) in enumerate(
            (
                (inner_place, inner_hbm),
                (far, main_hbm),
                (outer_place, relay_hbm),
                (outer_place, outer_hbm),
            )
        )
    ]
    copies[0].start()
    copies[1].start()

    @pl.when(relayed)
    def _():
        copies[2].start()
        copies[2].wait()

    @pl.when(jnp.logical_not(relayed))
    def _():
        copies[3].start()
        copies[3].wait()

    copies[0].wait()
    copies[1].wait()
    for q in range(far):
        for x in (q, span - 1 - q):
            pot[x] = inside[skip + x] * main[0, x]

    def step(s, carry):
        for row in (s + far, span - 1 - far - s):
            pot[row] = inside[skip + row] * main[0, row]
        for first in (s, span - 1 - far - s):
            for q in range(far + 1):
                x = first + q
                shift_row(
                    pot, dy_ref, sy_ref, x, skip + x, lambda side, block: strip_track[s, side, :, block]
                )

        def known():
            for q, row in enumerate((s + far + 1, span - 2 - far - s)):
                pot[row] = track[s, q, 0]
                dy_ref[row] = track[s, q, 1]

        if before < cells // 2:
            pl.when(s < cells // 2 + before)(known)
        else:
            known()
        if not last:
            for q, row in enumerate((s + 1, span - 2 - s)):
                track_out[s, q, 0] = pot[row]
                track_out[s, q, 1] = dy_ref[row]

        def diffuse(x):
            u = main[0, x]
            flow = row_spread(weight_ref, pot, dy_ref, sy_ref, x) - u * total[skip + x]
            main[0, x] = u + inside[skip + x] * flow

        for side, first in enumerate((s + 1, span - 1 - far - s)):
            for q in range(far):
                x = first + q
                if before < cells // 2 and q == (far - 1, 0)[side]:
                    pl.when((x < span // 2, x >= span // 2)[side])(functools.partial(diffuse, x))
                else:
                    diffuse(x)
        if not last:
            finished(main, main_out, out_sems, s, False)

        def react_pair(k, carry):
            near_row, far_row = s + 1 + k, span - 2 - s - k
            react_rows(main, inside.at[pl.ds(skip, span)], pot, (near_row, far_row))
            return carry

        lax.fori_loop(0, jnp.where(s < STEPS - 1, far, 0), react_pair, 0)
        return carry

    lax.fori_loop(0, STEPS, step, 0)
    if last:
        copies = [pltpu.make_async_copy(main.at[:, pl.ds(cells, cells)], out_hbm, sems.at[0])]
    else:
        rest = span - 2 * STEPS
        copies = [
            pltpu.make_async_copy(
                main.at[:, pl.ds(STEPS, rest)], main_out.at[:, pl.ds(STEPS, rest)], sems.at[0]
            )
        ] * (rest > 0)
    for copy in copies:
        copy.start()
    for copy in copies:
        copy.wait()
    if not last:

        def drained(s, carry):
            finished(main, main_out, out_sems, s, True)
            return carry

        lax.fori_loop(0, STEPS, drained, 0)


def shards(state, tissue_mask, layer_index, fibre):
    comps, cells, depth, width = state.shape
    across, along = lax.axis_size("gx"), lax.axis_size("gy")
    span = 3 * cells
    f32 = jnp.float32

    def swaps(size, first):
        pairs = [(i, i + 1) for i in range(first, size - 1, 2)]
        return pairs + [(j, i) for i, j in pairs]

    def both(inner, outer, axis, size):
        outer = lax.ppermute(outer, axis, swaps(size, 1))
        return lax.ppermute(inner, axis, swaps(size, 0)), outer

    def shape(*sizes):
        return jax.ShapeDtypeStruct(sizes, f32)

    vmem = pl.BlockSpec(memory_space=pltpu.VMEM)
    hbm = pl.BlockSpec(memory_space=pl.ANY)
    params = pltpu.CompilerParams(vmem_limit_bytes=12 << 20)

    def cost(rows):
        work = int(rows * depth * width * 350)
        return pl.CostEstimate(flops=work, bytes_accessed=8 << 20, transcendentals=0)

    *faces, edge = pl.pallas_call(
        functools.partial(first_kernel, CHUNKS),
        out_shape=[shape(comps, rows, depth, width) for rows in CHUNKS for _ in range(2)]
        + [shape(comps + 2, depth, LANES)],
        in_specs=[vmem, vmem],
        out_specs=[hbm] * (2 * len(CHUNKS)) + [vmem],
        scratch_shapes=[
            pltpu.VMEM((comps, cells, depth, width), f32),
            pltpu.VMEM((cells, depth, width), f32),
            pltpu.SemaphoreType.DMA((2 * len(CHUNKS),)),
        ],
        compiler_params=params,
        name="first",
    )(state, tissue_mask.transpose(0, 2, 1))
    inner_faces, outer_faces = faces[0::2], faces[1::2]
    edge_inner, edge_outer = both(edge, edge, "gy", along)
    odd_along = lax.rem(lax.axis_index("gy"), 2) == 1
    edge_before = jnp.where(odd_along, edge_inner, edge_outer)
    edge_after = jnp.where(odd_along, edge_outer, edge_inner)
    outer = lax.broadcasted_iota(jnp.int32, edge.shape, 2) % GROUP < EDGE
    strips = jnp.concatenate(
        [
            jnp.where(outer, edge_before, edge)[:-1],
            jnp.where(outer, edge, edge_after)[:-1],
            edge[-1:],
        ]
    )
    strip_inner, strip_outer = both(strips, strips, "gx", across)
    halos = [both(inner_faces[0], outer_faces[0], "gx", across)]
    bounds = [i for i in range(PLANE - 1, across - 1, PLANE)]
    close = [pair for pair in swaps(across, 1) if pair[0] // PLANE == pair[1] // PLANE]
    around = [(i, i - PLANE + 1) for i in bounds] + [(i + 1, i + PLANE) for i in bounds]
    onward = [(i - PLANE + 1, i + 1) for i in bounds] + [(i + PLANE, i) for i in bounds]
    far_outer = lax.ppermute(outer_faces[1], "gx", close + around)
    far_inner = lax.ppermute(inner_faces[1], "gx", swaps(across, 0))
    far_relay = lax.ppermute(far_outer, "gx", onward)
    halos.append((far_inner, far_outer, far_relay))

    weights = level_weights(layer_tensor(layer_index, fibre), 3 * LANES)
    inside, total, strip_track = pl.pallas_call(
        strip_kernel,
        out_shape=[
            shape(span, depth, width),
            shape(span, depth, width),
            shape(STEPS, 2, depth, 3 * LANES),
        ],
        in_specs=[hbm] * 3 + [vmem],
        out_specs=[vmem] * 3,
        scratch_shapes=[
            pltpu.VMEM((span, depth, width), f32),
            pltpu.VMEM((span, depth, width), f32),
            pltpu.VMEM((2, comps + 1, depth, 3 * LANES), f32),
            pltpu.VMEM((3, depth, LANES), f32),
            pltpu.VMEM((2, depth, 3 * LANES), f32),
            pltpu.SemaphoreType.DMA((9,)),
        ],
        compiler_params=params,
        cost_estimate=cost(30),
        name="strips",
    )(strip_inner, strips, strip_outer, weights)
    shared = (inside, total, strip_track)

    def buffers(count):
        return [pltpu.VMEM((comps, count, depth, width), f32)] + [
            pltpu.VMEM((count, depth, width), f32) for _ in range(3)
        ]

    track_shape = shape(STEPS, 2, 2, depth, width)
    near = CHUNKS[0]
    count = cells + 2 * near
    main, track = pl.pallas_call(
        functools.partial(near_kernel, len(CHUNKS), near),
        out_shape=[shape(comps, count, depth, width), track_shape],
        in_specs=[hbm] * (2 + len(CHUNKS)) + [vmem] * 4,
        out_specs=[hbm, vmem],
        scratch_shapes=buffers(count)
        + [pltpu.SemaphoreType.DMA((2 + len(CHUNKS),)), pltpu.SemaphoreType.DMA((2 * STEPS,))],
        compiler_params=params,
        cost_estimate=cost(70),
        name="near",
    )(*halos[0], *inner_faces, *shared, weights)
    for i, rows in enumerate(CHUNKS[1:], 1):
        last = i == len(CHUNKS) - 1
        count += 2 * rows
        outs = [shape(*state.shape)] if last else [shape(comps, count, depth, width), track_shape]
        result = pl.pallas_call(
            functools.partial(ring_kernel, last),
            out_shape=outs,
            in_specs=[hbm] * 4 + [vmem] * 5,
            out_specs=[hbm, vmem][: len(outs)],
            scratch_shapes=buffers(count)
            + [pltpu.SemaphoreType.DMA((4,))]
            + ([] if last else [pltpu.SemaphoreType.DMA((2 * STEPS,))]),
            compiler_params=params,
            cost_estimate=cost(18 * rows),
        )(halos[i][0], main, *halos[i][1:], *shared, track, weights)
        main, track = result if not last else (result[0], None)
    return main


def solution(mesh):
    placed = (P(None, "gx", None, "gy"), P("gx", None, "gy"), P(), P())

    return jax.shard_map(
        shards, mesh=mesh, in_specs=placed, out_specs=P(None, "gx", None, "gy"), check_vma=False
    )
```

```python
import functools
import math

import jax
import jax.numpy as jnp
from jax import lax
from jax.experimental import pallas as pl
from jax.experimental.pallas import tpu as pltpu
from jax.sharding import PartitionSpec as P


STEPS = 8
COMPS = 12
CHUNKS = (4, 4)
PLANE = 8
EDGE = 8
GROUP = 2 * EDGE
LANES = 128

time_step = 0.02
thermal_volt = 8314.472 * 310.0 / 96485.3415
potassium_out = 5.4
sodium_out = 140.0
calcium_out = 2.0
potassium_in = 138.3
sodium_in = 7.67
transverse = 0.04
longitudinal = 0.12
LOG2E = math.log2(math.e)


def react(state):
    (x, act, inact, slow, calact, calinact, tract, trinact, rapact, rapinact, slowact, calcium) = state

    def power(rate, offset=0.0, scale=1.0):
        shift = offset * LOG2E + math.log2(scale)
        scaled = x * (100.0 * rate * LOG2E)
        return jnp.exp2(scaled + shift if shift else scaled)

    def bell(centre, width, scale):
        root = math.sqrt(LOG2E / width)
        away = x * (100.0 * root) + centre * root
        return jnp.exp2(math.log2(scale) - away * away)

    def step(rate, offset):
        return jax.nn.sigmoid(x * (100.0 * rate) + offset)

    def inverse(value):
        return 1.0 / value

    def moved(gate, steady, exponent):
        return steady + (gate - steady) * jnp.exp2(exponent)

    e = math.exp
    speed = time_step * LOG2E
    voltage = 100.0 * x
    rev_potassium = thermal_volt * math.log(potassium_out / potassium_in)
    rev_sodium = thermal_volt * math.log(sodium_out / sodium_in)
    rev_slow = thermal_volt * math.log(
        (potassium_out + 0.03 * sodium_out) / (potassium_in + 0.03 * sodium_in)
    )
    up20 = power(1 / 20)
    up10 = up20 * up20
    up5 = up10 * up10
    down20 = power(-1 / 20)
    down10 = down20 * down20
    down5 = down10 * down10
    up15 = power(1 / 15)
    down6 = power(-1 / 6)
    down14 = power(-1 / 14)
    down7 = down14 * down14
    fall = jnp.exp2(jnp.minimum(x * (-50.0 * LOG2E) - 20.0 * LOG2E, 120.0))
    minus_upper = inverse(-1.0 - fall)
    minus_lower = fall * minus_upper

    above = voltage - rev_potassium
    cam = jnp.maximum(calcium, 0.02)
    past_calcium = (voltage - 0.5 * thermal_volt * math.log(calcium_out / 0.001)) + (
        0.5 * thermal_volt
    ) * jnp.log(cam)
    past_sodium = voltage - rev_sodium
    inward_x = 1.0 + power(0.06, -0.06 * (rev_potassium + 200.0))
    inward_y = 1.0 + fall * e(20.0 + 0.5 * rev_potassium)
    inward_b = power(0.0002, 0.0002 * (100.0 - rev_potassium), 30.0) + up10 * (
        10.0 * e(-0.1 * rev_potassium - 1.0)
    )
    inward = (5.405 * inward_y) * inverse(inward_y + inward_b * inward_x)
    plateau = inverse(1.0 / 0.0146 + power(-1 / 5.98, 25.0 / 5.98, 1.0 / 0.0146))
    full = power(-1.0 / thermal_volt)
    pump_top = 2.724 * potassium_out / (potassium_out + 1.0) * sodium_in / (sodium_in + 40.0)
    pump = inverse(
        (power(-0.1 / thermal_volt, 0.0, 0.1245 / pump_top) + 1.0 / pump_top)
        + full * (0.0353 / pump_top)
    )
    whole = 1000.0 / ((87.5**3 + sodium_out**3) * (1.38 + calcium_out))
    inner = whole * sodium_in**3 * calcium_out
    exchange = (inner - (cam * (2.5 * 0.001 * whole * sodium_out**3)) * full) * inverse(
        power(-0.35 / thermal_volt) + 0.1 * full
    )
    pump_calcium = 0.1238 - 0.0619 * inverse(cam + 0.5)
    calcium_sum = (0.08 * calact * calinact + 0.000592) * past_calcium + pump_calcium
    ionic = (
        (14.838 * act * (act * act) * inact * slow + 0.00029) * past_sodium
        + calcium_sum
        + (0.294 * tract * trinact + 0.153 * rapact * rapinact + inward + plateau) * above
        + (0.392 * slowact * slowact) * (voltage - rev_slow)
        + pump
        + exchange
    )
    new_x = x - (time_step / 100.0) * ionic
    new_calcium = calcium - (time_step * 0.05) * (calcium_sum - 2.0 * exchange)

    a = up5 * (e(7.0))
    b = power(1 / 200, -0.25)
    root = step(1 / 9.03, 56.86 / 9.03)
    rate = ((a * (-10.0 * speed) - (1.0 + e(-5.0)) * 10.0 * speed) - down5 * (e(-12.0) * 10.0 * speed)) * (
        (1.0 + b) * inverse(2.0 + a + b)
    )
    new_act = moved(act, root * root, rate)

    root = step(-1 / 7.43, -71.55 / 7.43)
    steady = root * root
    rate = minus_lower * (
        power(-1 / 6.8, -80.0 / 6.8, 0.057 * speed)
        + power(0.079, 0.0, 2.7 * speed)
        + power(0.3485, 0.0, 310000.0 * speed)
    ) + minus_upper * inverse(
        1.0 / (0.77 / 0.13 * speed) + power(-1 / 11.1, -10.66 / 11.1, 1.0 / (0.77 / 0.13 * speed))
    )
    new_inact = moved(inact, steady, rate)
    rate = minus_lower * (
        power(-0.01052, 0.0, 0.02424 * speed) * step(0.1378, 0.1378 * 40.14)
        - (power(0.2444, 0.0, 25428.0 * speed) + power(-0.04391, 0.0, 6.948e-06 * speed))
        * ((voltage + 37.78) * step(-0.311, -0.311 * 79.23))
    ) + minus_upper * (
        power(0.057) * inverse(1.0 / (0.6 * speed) + down10 * (e(-3.2) / (0.6 * speed)))
    )
    new_slow = moved(slow, steady, rate)

    p = 1.0 + power(-1 / 13, -35.0 / 13)
    r = down20 * (-speed * e(2.5)) - speed
    pq = p * (1.0 + up5 * e(1.0))
    rate = pq * (r * inverse((-1.96 / speed - (0.35 / speed) * p) * r + pq))
    new_calact = moved(calact, step(1 / 7.5, 8.0 / 7.5), rate)

    b = up10 * (-speed * e(3.0))
    den = (down10 * (-speed * e(1.3)) - speed * (1.0 + e(4.3))) + b
    rate = den * inverse(
        (380.0 - 180.0 * (1.0 + e(4.3)) - (20.0 / speed) * b)
        - (bell(27.0, 225.0, 1102.5 / speed) + 200.0 / speed) * den
    )
    new_calinact = moved(calinact, down7 * inverse(down7 + e(20.0 / 7)), rate)

    rate = inverse(-0.8 / speed - bell(40.0, 1800.0, 9.5 / speed))
    new_tract = moved(tract, inverse(1.0 + down6 * e(20.0 / 6)), rate)

    t = up5 * (-speed * e(-4.0)) - speed
    rate = t * inverse(5.0 - (bell(45.0, 320.0, 85.0 / speed) + 3.0 / speed) * t)
    new_trinact = moved(trinact, inverse(1.0 + up5 * e(4.0)), rate)

    rate = (down10 * (-speed * e(-4.5) / 2700.0) - speed / 2700.0) * (
        1.0 + power(1 / 11.5, 30.0 / 11.5)
    )
    new_rapact = moved(rapact, inverse(1.0 + down7 * e(-26.0 / 7)), rate)

    rate = (up20 + down20) * (-speed * e(-3.0) / 3.36) - speed * (1.0 + e(-6.0)) / 3.36
    new_rapinact = moved(rapinact, step(-1 / 24, -88.0 / 24), rate)

    y = up15 * (-speed * e(-35.0 / 15)) - speed
    rate = y * inverse(
        lax.rsqrt(1.0 / 1400.0**2 + down6 * (e(5.0 / 6) / 1400.0**2)) - (80.0 / speed) * y
    )
    new_slowact = moved(slowact, inverse(1.0 + down14 * e(-5.0 / 14)), rate)
    return (
        new_x,
        new_act,
        new_inact,
        new_slow,
        new_calact,
        new_calinact,
        new_tract,
        new_trinact,
        new_rapact,
        new_rapinact,
        new_slowact,
        new_calcium,
    )


def layer_tensor(layer_index, fibre):
    angle_in = fibre[0]
    angle_out = fibre[1]
    fibre_x = jnp.cos(angle_in) * jnp.cos(angle_out)
    fibre_y = jnp.sin(angle_in) * jnp.cos(angle_out)
    fibre_z = jnp.sin(angle_out)
    spread = longitudinal - transverse
    tensor_table = jnp.stack(
        [
            transverse + spread * fibre_x * fibre_x,
            transverse + spread * fibre_y * fibre_y,
            transverse + spread * fibre_z * fibre_z,
            spread * fibre_x * fibre_y,
            spread * fibre_x * fibre_z,
            spread * fibre_y * fibre_z,
        ]
    )
    layer_ids = jnp.arange(fibre.shape[1], dtype=jnp.int32)
    chosen = layer_index[:, None] == layer_ids[None, :]
    return jnp.sum(jnp.where(chosen[None], tensor_table[:, None, :], jnp.float32(0.0)), axis=2)


def level_weights(tensor, lanes):
    between = (tensor[:, 1:] + tensor[:, :-1]) / 2.0
    upward = jnp.pad(between, ((0, 0), (0, 1)))
    downward = jnp.pad(between, ((0, 0), (1, 0)))
    rows = jnp.stack(
        [
            tensor[0],
            tensor[1],
            tensor[3] / 2.0,
            upward[2],
            upward[4] / 2.0,
            upward[5] / 2.0,
            downward[2],
            downward[4] / 2.0,
            downward[5] / 2.0,
        ]
    )
    return jnp.broadcast_to(rows[:, :, None], rows.shape + (lanes,))


def first_kernel(chunks, state_ref, mask_ref, *refs):
    faces, (edge_ref, main, inside, sems) = refs[: 2 * len(chunks)], refs[2 * len(chunks) :]
    cells, depth, width = state_ref.shape[1:]
    odd = lax.rem(lax.axis_index("gx"), 2)
    lane = lax.broadcasted_iota(jnp.int32, (depth, LANES), 1)
    diagonal = lax.broadcasted_iota(jnp.int32, (depth, depth), 0) == lax.broadcasted_iota(
        jnp.int32, (depth, depth), 1
    )
    codes = jnp.zeros((depth, LANES), jnp.float32)
    for x in range(cells):
        for b in range(width // LANES):
            code = jnp.where(mask_ref[x, b : b + 1, :] > 0, jnp.float32(1.0), jnp.float32(0.0))
            code = jnp.where(diagonal, jnp.broadcast_to(code, (depth, depth)), jnp.float32(0.0))
            code = jnp.broadcast_to(jnp.sum(code, axis=1, keepdims=True), (depth, LANES))
            inside[x, :, pl.ds(b * LANES, LANES)] = code
            codes = jnp.where(lane == 2 * x + b, code, codes)
    edge_ref[COMPS + 1] = codes

    def react_pair(k, carry):
        for x in (2 * k, 2 * k + 1):
            for level in range(depth // 8):
                for i in range(width // LANES):
                    place = (x, pl.ds(level * 8, 8), pl.ds(i * LANES, LANES))
                    old = [state_ref[(c,) + place] for c in range(COMPS)]
                    live = inside[place] > 0.5
                    for c, new in enumerate(react(old)):
                        main[(c,) + place] = jnp.where(live, new, old[c])
        return carry

    lax.fori_loop(0, cells // 2, react_pair, 0)
    copies = []
    start = 0
    for i, rows in enumerate(chunks):
        above, below = cells - start - rows, start
        inner = above + odd * (below - above)
        outer = below + odd * (above - below)
        for face, row, sem in ((faces[2 * i], inner, 2 * i), (faces[2 * i + 1], outer, 2 * i + 1)):
            copies.append(pltpu.make_async_copy(main.at[:, pl.ds(row, rows)], face, sems.at[sem]))
        start += rows
    for copy in copies:
        copy.start()

    def packed(first, last):
        total = jnp.zeros((depth, LANES), jnp.float32)
        for i in range(cells):
            joined = jnp.where(lane < EDGE, first(i), last(i))
            turned = pltpu.roll(joined, i * GROUP + EDGE, 1)
            total = jnp.where(lane // GROUP == i, turned, total)
        return total

    def some(k, carry):
        for q in range(3):
            c = 3 * k + q
            edge_ref[c] = packed(
                lambda i: main[c, i, :, :LANES], lambda i: main[c, i, :, width - LANES :]
            )
        return carry

    lax.fori_loop(0, COMPS // 3, some, 0)
    edge_ref[COMPS] = packed(
        lambda i: inside[i, :, :LANES], lambda i: inside[i, :, width - LANES :]
    )
    for copy in copies:
        copy.wait()


def react_tile(at, live, kept=COMPS):
    new = react([at(c)[...] for c in range(COMPS)])
    for c in range(kept):
        pltpu.store(at(c), new[c], mask=live > 0.5)
    return live * new[0]


def react_rows(main, inside, pot, rows, kept=COMPS):
    for x in rows:
        for level in range(main.shape[2] // 8):
            for i in range(main.shape[3] // LANES):
                place = (x, pl.ds(level * 8, 8), pl.ds(i * LANES, LANES))
                pot[place] = react_tile(lambda c: main.at[(c,) + place], inside[place], kept)


def shift_row(pot, dy_ref, sy_ref, x, ext, strip_row):
    shape = (pot.shape[1], LANES)
    lane = lax.broadcasted_iota(jnp.int32, shape, 1)
    first_lane, last_lane = lane == 0, lane == LANES - 1
    block = pl.ds(pl.multiple_of(ext // 8 * LANES, LANES), LANES)
    place = lax.rem(ext, 8) * GROUP
    before = pltpu.roll(strip_row(0, block), lax.rem(2 * LANES - place - (EDGE - 1), LANES), 1)
    after = pltpu.roll(strip_row(1, block), lax.rem(2 * LANES - 1 - place - EDGE, LANES), 1)
    near, far = pot[x, :, :LANES], pot[x, :, LANES:]
    near_up, far_up = pltpu.roll(near, 1, 1), pltpu.roll(far, 1, 1)
    near_down, far_down = pltpu.roll(near, LANES - 1, 1), pltpu.roll(far, LANES - 1, 1)
    lower = jnp.where(first_lane, before, near_up)
    upper = jnp.where(last_lane, far_down, near_down)
    dy_ref[x, :, :LANES] = upper - lower
    sy_ref[x, :, :LANES] = upper + lower
    lower = jnp.where(first_lane, near_up, far_up)
    upper = jnp.where(last_lane, after, far_down)
    dy_ref[x, :, LANES:] = upper - lower
    sy_ref[x, :, LANES:] = upper + lower


def spread(weight_ref, p, dx, sx, dy, sy, cross):
    depth, lanes = p.shape
    w = [weight_ref[i, :, :lanes] for i in range(9)]
    rising = w[3] * p - w[4] * dx - w[5] * dy
    falling = w[6] * p + w[7] * dx + w[8] * dy
    return (
        w[0] * sx
        + w[1] * sy
        + w[2] * cross
        + pltpu.roll(rising, 1, 0)
        + pltpu.roll(falling, depth - 1, 0)
    )


def row_spread(weight_ref, pot, dy_ref, sy_ref, x):
    before, after = pot[x - 1], pot[x + 1]
    return spread(
        weight_ref,
        pot[x],
        after - before,
        after + before,
        dy_ref[x],
        sy_ref[x],
        dy_ref[x + 1] - dy_ref[x - 1],
    )


def strip_spread(weight_ref, p):
    long = p.shape[1]
    lower, upper = pltpu.roll(p, 1, 1), pltpu.roll(p, long - 1, 1)
    before, after = pltpu.roll(p, GROUP, 1), pltpu.roll(p, long - GROUP, 1)
    dy = upper - lower
    cross = pltpu.roll(dy, long - GROUP, 1) - pltpu.roll(dy, GROUP, 1)
    return spread(weight_ref, p, after - before, after + before, dy, upper + lower, cross)


def strip_kernel(
    strip_inner_hbm,
    strip_hbm,
    strip_outer_hbm,
    weight_ref,
    inside,
    total,
    strip_track,
    dy_ref,
    sy_ref,
    strip,
    code_ref,
    strip_total,
    sems,
):
    span, depth, width = inside.shape
    cells = span // 3
    odd = lax.rem(lax.axis_index("gx"), 2)
    sides = (0, 1)
    copies = []
    for q, (i, source) in enumerate(
        ((2 - 2 * odd, strip_inner_hbm), (1, strip_hbm), (2 * odd, strip_outer_hbm))
    ):
        part = pl.ds(pl.multiple_of(i * LANES, LANES), LANES)
        for side in sides:
            held = source.at[pl.ds(side * (COMPS + 1), COMPS + 1)]
            copies.append(
                pltpu.make_async_copy(held, strip.at[side, :, :, part], sems.at[3 * q + side])
            )
        copies.append(
            pltpu.make_async_copy(
                source.at[pl.ds(2 * (COMPS + 1), 1)], code_ref.at[pl.ds(i, 1)], sems.at[3 * q + 2]
            )
        )
    for copy in copies:
        copy.start()
    for copy in copies:
        copy.wait()
    for i in range(3):
        codes = code_ref[i]
        for x in range(cells):
            for b in range(width // LANES):
                value = jnp.broadcast_to(codes[:, 2 * x + b : 2 * x + b + 1], (depth, LANES))
                inside[i * cells + x, :, b * LANES : (b + 1) * LANES] = value

    def shift_mask(k, carry):
        for q in range(4):
            x = 4 * k + q
            shift_row(inside, dy_ref, sy_ref, x, x, lambda side, block: strip[side, COMPS, :, block])
        return carry

    lax.fori_loop(0, span // 4, shift_mask, 0)

    def total_rows(k, carry):
        for q in range(2):
            x = 1 + 2 * k + q
            total[x] = row_spread(weight_ref, inside, dy_ref, sy_ref, x)
        return carry

    lax.fori_loop(0, span // 2 - 1, total_rows, 0)
    for side in sides:
        strip_total[side] = strip_spread(weight_ref, strip[side, COMPS])
        strip_track[0, side] = strip[side, COMPS] * strip[side, 0]

    def step(kept, s, carry):
        for side in sides:
            u = strip[side, 0]
            flow = strip_spread(weight_ref, strip_track[s, side]) - u * strip_total[side]
            strip[side, 0] = u + strip[side, COMPS] * flow

        for side in sides:
            for level in range(depth // 8):
                for i in range(3):
                    place = (pl.ds(level * 8, 8), pl.ds(i * LANES, LANES))
                    held = react_tile(
                        lambda c: strip.at[(side, c) + place], strip[(side, COMPS) + place], kept
                    )
                    strip_track[(s + 1, side) + place] = held
        return carry

    lax.fori_loop(0, STEPS - 2, functools.partial(step, COMPS), 0)
    step(1, STEPS - 2, 0)


def finished(main, main_out, sems, s, wait):
    count = main.shape[1]
    for q, row in enumerate((s, count - 1 - s)):
        copy = pltpu.make_async_copy(
            main.at[:, pl.ds(row, 1)], main_out.at[:, pl.ds(row, 1)], sems.at[2 * s + q]
        )
        if wait:
            copy.wait()
        else:
            copy.start()


def near_kernel(pieces, near, *refs):
    sources, refs = refs[: pieces + 2], refs[pieces + 2 :]
    inside, total, strip_track, weight_ref, main_out, track = refs[:6]
    main, pot, dy_ref, sy_ref, sems, out_sems = refs[6:]
    count, _, _ = pot.shape
    cells = count - 2 * near
    skip = cells - near
    odd = lax.rem(lax.axis_index("gx"), 2)
    inner_hbm, outer_hbm = sources[:2]
    places = [(near + cells - odd * (near + cells), inner_hbm), (odd * (near + cells), outer_hbm)]
    start = 0
    for source in sources[2:]:
        rows = source.shape[1]
        above, below = cells - start - rows, start
        places.append((near + above + odd * (below - above), source))
        start += rows
    copies = [
        pltpu.make_async_copy(source, main.at[:, pl.ds(row, source.shape[1])], sems.at[i])
        for i, (row, source) in enumerate(places)
    ]
    for copy in copies:
        copy.start()
    for copy in copies:
        copy.wait()

    group = 4 if count % 4 == 0 else 2

    def start_row(k, carry):
        for q in range(2):
            pot[2 * k + q] = inside[skip + 2 * k + q] * main[0, 2 * k + q]
        return carry

    lax.fori_loop(0, count // 2, start_row, 0)

    def shift(s, x):
        shift_row(
            pot, dy_ref, sy_ref, x, skip + x, lambda side, block: strip_track[s, side, :, block]
        )

    def shift_some(k, carry):
        for q in range(group):
            shift(0, group * k + q)
        return carry

    lax.fori_loop(0, count // group, shift_some, 0)

    def step(s, carry):
        for q, row in enumerate((s + 1, count - 2 - s)):
            track[s, q, 0] = pot[row]
            track[s, q, 1] = dy_ref[row]

        def diffuse_some(size, start, k, carry):
            for q in range(size):
                x = start + size * k + q
                u = main[0, x]
                flow = row_spread(weight_ref, pot, dy_ref, sy_ref, x) - u * total[skip + x]
                main[0, x] = u + inside[skip + x] * flow
            return carry

        pairs = jnp.maximum(count // 2 - 1 - s, 0)
        lax.fori_loop(0, pairs // 2, functools.partial(diffuse_some, 4, s + 1), 0)
        rest = s + 1 + pairs // 2 * 4
        lax.fori_loop(0, lax.rem(pairs, 2), functools.partial(diffuse_some, 2, rest), 0)

        @pl.when(s < min(STEPS, count // 2))
        def _():
            finished(main, main_out, out_sems, s, False)

        def react_some(k, carry):
            x = s + 1 + 2 * k
            for q in range(2):
                shift(s + 1, jnp.maximum(x - 2 + q, 0))
            react_rows(main, inside.at[pl.ds(skip, count)], pot, (x, x + 1))
            return carry

        @pl.when(s < min(STEPS - 1, count // 2 - 1))
        def _():
            lax.fori_loop(0, count // 2 - 1 - s, react_some, 0)
            for q in range(2):
                shift(s + 1, count - 3 - s + q)

        return carry

    lax.fori_loop(0, STEPS, step, 0)

    def drained(s, carry):
        finished(main, main_out, out_sems, s, True)
        return carry

    lax.fori_loop(0, min(STEPS, count // 2), drained, 0)


def ring_kernel(last, *refs):
    inner_hbm, main_hbm, outer_hbm, relay_hbm = refs[:4]
    inside, total, strip_track, track, weight_ref = refs[4:9]
    if last:
        out_hbm, main, pot, dy_ref, sy_ref, sems = refs[9:]
    else:
        main_out, track_out, main, pot, dy_ref, sy_ref, sems, out_sems = refs[9:]
    far, _, _ = inner_hbm.shape[1:]
    count = main_hbm.shape[1]
    span = far + count + far
    cells = inside.shape[0] // 3
    skip = (inside.shape[0] - span) // 2
    before = (count - cells) // 2
    odd = lax.rem(lax.axis_index("gx"), 2)
    across = lax.rem(lax.axis_index("gx") + 1, PLANE)
    relayed = jnp.logical_or(across == 0, across == 1)
    inner_place, outer_place = far + count - odd * (far + count), odd * (far + count)
    copies = [
        pltpu.make_async_copy(source, main.at[:, pl.ds(row, source.shape[1])], sems.at[i])
        for i, (row, source) in enumerate(
            (
                (inner_place, inner_hbm),
                (far, main_hbm),
                (outer_place, relay_hbm),
                (outer_place, outer_hbm),
            )
        )
    ]
    copies[0].start()
    copies[1].start()

    @pl.when(relayed)
    def _():
        copies[2].start()
        copies[2].wait()

    @pl.when(jnp.logical_not(relayed))
    def _():
        copies[3].start()
        copies[3].wait()

    copies[0].wait()
    copies[1].wait()
    for q in range(far):
        for x in (q, span - 1 - q):
            pot[x] = inside[skip + x] * main[0, x]

    def shift(s, x):
        shift_row(
            pot, dy_ref, sy_ref, x, skip + x, lambda side, block: strip_track[s, side, :, block]
        )

    for q in range(far - 1):
        for x in (q, span - 1 - q):
            shift(0, x)

    def step(s, carry):
        for row in (s + far, span - 1 - far - s):
            pot[row] = inside[skip + row] * main[0, row]
        for q in (far - 1, far):
            for x in (s + q, span - 1 - s - q):
                shift(s, x)

        def known():
            for q, row in enumerate((s + far + 1, span - 2 - far - s)):
                pot[row] = track[s, q, 0]
                dy_ref[row] = track[s, q, 1]

        if before < cells // 2:
            pl.when(s < cells // 2 + before)(known)
        else:
            known()
        if not last:
            for q, row in enumerate((s + 1, span - 2 - s)):
                track_out[s, q, 0] = pot[row]
                track_out[s, q, 1] = dy_ref[row]

        def diffuse(x):
            u = main[0, x]
            flow = row_spread(weight_ref, pot, dy_ref, sy_ref, x) - u * total[skip + x]
            main[0, x] = u + inside[skip + x] * flow

        for side, first in enumerate((s + 1, span - 1 - far - s)):
            for q in range(far):
                x = first + q
                if before < cells // 2 and q == (far - 1, 0)[side]:
                    pl.when((x < span // 2, x >= span // 2)[side])(functools.partial(diffuse, x))
                else:
                    diffuse(x)
        if not last:
            finished(main, main_out, out_sems, s, False)

        held = inside.at[pl.ds(skip, span)]

        def react_pair(k, carry):
            near_row, far_row = s + 1 + k, span - 2 - s - k
            shift(s + 1, near_row - 1)
            shift(s + 1, far_row + 1)
            react_rows(main, held, pot, (near_row, far_row))
            return carry

        @pl.when(s < STEPS - 1)
        def _():
            react_rows(main, held, pot, (s + 1, span - 2 - s), 1 if last else COMPS)
            lax.fori_loop(1, far, react_pair, 0)

        return carry

    lax.fori_loop(0, STEPS, step, 0)
    if last:
        copies = [pltpu.make_async_copy(main.at[:, pl.ds(cells, cells)], out_hbm, sems.at[0])]
    else:
        rest = span - 2 * STEPS
        copies = [
            pltpu.make_async_copy(
                main.at[:, pl.ds(STEPS, rest)], main_out.at[:, pl.ds(STEPS, rest)], sems.at[0]
            )
        ] * (rest > 0)
    for copy in copies:
        copy.start()
    for copy in copies:
        copy.wait()
    if not last:

        def drained(s, carry):
            finished(main, main_out, out_sems, s, True)
            return carry

        lax.fori_loop(0, STEPS, drained, 0)


def shards(state, tissue_mask, layer_index, fibre):
    comps, cells, depth, width = state.shape
    across, along = lax.axis_size("gx"), lax.axis_size("gy")
    span = 3 * cells
    f32 = jnp.float32

    def swaps(size, first):
        pairs = [(i, i + 1) for i in range(first, size - 1, 2)]
        return pairs + [(j, i) for i, j in pairs]

    def both(inner, outer, axis, size):
        outer = lax.ppermute(outer, axis, swaps(size, 1))
        return lax.ppermute(inner, axis, swaps(size, 0)), outer

    def shape(*sizes):
        return jax.ShapeDtypeStruct(sizes, f32)

    vmem = pl.BlockSpec(memory_space=pltpu.VMEM)
    hbm = pl.BlockSpec(memory_space=pl.ANY)
    params = pltpu.CompilerParams(vmem_limit_bytes=12 << 20)

    def cost(rows):
        work = int(rows * depth * width * 350)
        return pl.CostEstimate(flops=work, bytes_accessed=8 << 20, transcendentals=0)

    *faces, edge = pl.pallas_call(
        functools.partial(first_kernel, CHUNKS),
        out_shape=[shape(comps, rows, depth, width) for rows in CHUNKS for _ in range(2)]
        + [shape(comps + 2, depth, LANES)],
        in_specs=[vmem, vmem],
        out_specs=[hbm] * (2 * len(CHUNKS)) + [vmem],
        scratch_shapes=[
            pltpu.VMEM((comps, cells, depth, width), f32),
            pltpu.VMEM((cells, depth, width), f32),
            pltpu.SemaphoreType.DMA((2 * len(CHUNKS),)),
        ],
        compiler_params=params,
        name="first",
    )(state, tissue_mask.transpose(0, 2, 1))
    inner_faces, outer_faces = faces[0::2], faces[1::2]
    edge_inner, edge_outer = both(edge, edge, "gy", along)
    odd_along = lax.rem(lax.axis_index("gy"), 2) == 1
    edge_before = jnp.where(odd_along, edge_inner, edge_outer)
    edge_after = jnp.where(odd_along, edge_outer, edge_inner)
    outer = lax.broadcasted_iota(jnp.int32, edge.shape, 2) % GROUP < EDGE
    strips = jnp.concatenate(
        [
            jnp.where(outer, edge_before, edge)[:-1],
            jnp.where(outer, edge, edge_after)[:-1],
            edge[-1:],
        ]
    )
    strip_inner, strip_outer = both(strips, strips, "gx", across)
    halos = [both(inner_faces[0], outer_faces[0], "gx", across)]
    bounds = [i for i in range(PLANE - 1, across - 1, PLANE)]
    close = [pair for pair in swaps(across, 1) if pair[0] // PLANE == pair[1] // PLANE]
    around = [(i, i - PLANE + 1) for i in bounds] + [(i + 1, i + PLANE) for i in bounds]
    onward = [(i - PLANE + 1, i + 1) for i in bounds] + [(i + PLANE, i) for i in bounds]
    far_outer = lax.ppermute(outer_faces[1], "gx", close + around)
    far_inner = lax.ppermute(inner_faces[1], "gx", swaps(across, 0))
    far_relay = lax.ppermute(far_outer, "gx", onward)
    halos.append((far_inner, far_outer, far_relay))

    weights = level_weights(layer_tensor(layer_index, fibre), 3 * LANES)
    inside, total, strip_track = pl.pallas_call(
        strip_kernel,
        out_shape=[
            shape(span, depth, width),
            shape(span, depth, width),
            shape(STEPS, 2, depth, 3 * LANES),
        ],
        in_specs=[hbm] * 3 + [vmem],
        out_specs=[vmem] * 3,
        scratch_shapes=[
            pltpu.VMEM((span, depth, width), f32),
            pltpu.VMEM((span, depth, width), f32),
            pltpu.VMEM((2, comps + 1, depth, 3 * LANES), f32),
            pltpu.VMEM((3, depth, LANES), f32),
            pltpu.VMEM((2, depth, 3 * LANES), f32),
            pltpu.SemaphoreType.DMA((9,)),
        ],
        compiler_params=params,
        cost_estimate=cost(30),
        name="strips",
    )(strip_inner, strips, strip_outer, weights)
    shared = (inside, total, strip_track)

    def buffers(count):
        return [pltpu.VMEM((comps, count, depth, width), f32)] + [
            pltpu.VMEM((count, depth, width), f32) for _ in range(3)
        ]

    track_shape = shape(STEPS, 2, 2, depth, width)
    near = CHUNKS[0]
    count = cells + 2 * near
    main, track = pl.pallas_call(
        functools.partial(near_kernel, len(CHUNKS), near),
        out_shape=[shape(comps, count, depth, width), track_shape],
        in_specs=[hbm] * (2 + len(CHUNKS)) + [vmem] * 4,
        out_specs=[hbm, vmem],
        scratch_shapes=buffers(count)
        + [pltpu.SemaphoreType.DMA((2 + len(CHUNKS),)), pltpu.SemaphoreType.DMA((2 * STEPS,))],
        compiler_params=params,
        cost_estimate=cost(70),
        name="near",
    )(*halos[0], *inner_faces, *shared, weights)
    for i, rows in enumerate(CHUNKS[1:], 1):
        last = i == len(CHUNKS) - 1
        count += 2 * rows
        outs = [shape(*state.shape)] if last else [shape(comps, count, depth, width), track_shape]
        result = pl.pallas_call(
            functools.partial(ring_kernel, last),
            out_shape=outs,
            in_specs=[hbm] * 4 + [vmem] * 5,
            out_specs=[hbm, vmem][: len(outs)],
            scratch_shapes=buffers(count)
            + [pltpu.SemaphoreType.DMA((4,))]
            + ([] if last else [pltpu.SemaphoreType.DMA((2 * STEPS,))]),
            compiler_params=params,
            cost_estimate=cost(18 * rows),
        )(halos[i][0], main, *halos[i][1:], *shared, track, weights)
        main, track = result if not last else (result[0], None)
    return main


def solution(mesh):
    placed = (P(None, "gx", None, "gy"), P("gx", None, "gy"), P(), P())

    return jax.shard_map(
        shards, mesh=mesh, in_specs=placed, out_specs=P(None, "gx", None, "gy"), check_vma=False
    )
```

```python
import functools
import math

import jax
import jax.numpy as jnp
from jax import lax
from jax.experimental import pallas as pl
from jax.experimental.pallas import tpu as pltpu
from jax.sharding import PartitionSpec as P


STEPS = 8
COMPS = 12
CHUNKS = (4, 4)
PLANE = 8
EDGE = 8
GROUP = 2 * EDGE
LANES = 128

time_step = 0.02
thermal_volt = 8314.472 * 310.0 / 96485.3415
potassium_out = 5.4
sodium_out = 140.0
calcium_out = 2.0
potassium_in = 138.3
sodium_in = 7.67
transverse = 0.04
longitudinal = 0.12
LOG2E = math.log2(math.e)


def react(state):
    (x, act, inact, slow, calact, calinact, tract, trinact, rapact, rapinact, slowact, calcium) = state

    def power(rate, offset=0.0, scale=1.0):
        shift = offset * LOG2E + math.log2(scale)
        scaled = x * (100.0 * rate * LOG2E)
        return jnp.exp2(scaled + shift if shift else scaled)

    def bell(centre, width, scale):
        root = math.sqrt(LOG2E / width)
        away = x * (100.0 * root) + centre * root
        return jnp.exp2(math.log2(scale) - away * away)

    def step(rate, offset):
        return jax.nn.sigmoid(x * (100.0 * rate) + offset)

    def inverse(value):
        return 1.0 / value

    def moved(gate, steady, exponent):
        return steady + (gate - steady) * jnp.exp2(exponent)

    e = math.exp
    speed = time_step * LOG2E
    voltage = 100.0 * x
    rev_potassium = thermal_volt * math.log(potassium_out / potassium_in)
    rev_sodium = thermal_volt * math.log(sodium_out / sodium_in)
    rev_slow = thermal_volt * math.log(
        (potassium_out + 0.03 * sodium_out) / (potassium_in + 0.03 * sodium_in)
    )
    up20 = power(1 / 20)
    up10 = up20 * up20
    up5 = up10 * up10
    down20 = power(-1 / 20)
    down10 = down20 * down20
    down5 = down10 * down10
    up15 = power(1 / 15)
    down6 = power(-1 / 6)
    down14 = power(-1 / 14)
    down7 = down14 * down14
    fall = jnp.exp2(jnp.minimum(x * (-50.0 * LOG2E) - 20.0 * LOG2E, 120.0))
    minus_upper = inverse(-1.0 - fall)
    minus_lower = fall * minus_upper

    above = voltage - rev_potassium
    cam = jnp.maximum(calcium, 0.02)
    past_calcium = (voltage - 0.5 * thermal_volt * math.log(calcium_out / 0.001)) + (
        0.5 * thermal_volt
    ) * jnp.log(cam)
    past_sodium = voltage - rev_sodium
    inward_x = 1.0 + power(0.06, -0.06 * (rev_potassium + 200.0))
    inward_y = 1.0 + fall * e(20.0 + 0.5 * rev_potassium)
    inward_b = power(0.0002, 0.0002 * (100.0 - rev_potassium), 30.0) + up10 * (
        10.0 * e(-0.1 * rev_potassium - 1.0)
    )
    inward = (5.405 * inward_y) * inverse(inward_y + inward_b * inward_x)
    plateau = inverse(1.0 / 0.0146 + power(-1 / 5.98, 25.0 / 5.98, 1.0 / 0.0146))
    full = power(-1.0 / thermal_volt)
    pump_top = 2.724 * potassium_out / (potassium_out + 1.0) * sodium_in / (sodium_in + 40.0)
    pump = inverse(
        (power(-0.1 / thermal_volt, 0.0, 0.1245 / pump_top) + 1.0 / pump_top)
        + full * (0.0353 / pump_top)
    )
    whole = 1000.0 / ((87.5**3 + sodium_out**3) * (1.38 + calcium_out))
    inner = whole * sodium_in**3 * calcium_out
    exchange = (inner - (cam * (2.5 * 0.001 * whole * sodium_out**3)) * full) * inverse(
        power(-0.35 / thermal_volt) + 0.1 * full
    )
    pump_calcium = 0.1238 - 0.0619 * inverse(cam + 0.5)
    calcium_sum = (0.08 * calact * calinact + 0.000592) * past_calcium + pump_calcium
    ionic = (
        (14.838 * act * (act * act) * inact * slow + 0.00029) * past_sodium
        + calcium_sum
        + (0.294 * tract * trinact + 0.153 * rapact * rapinact + inward + plateau) * above
        + (0.392 * slowact * slowact) * (voltage - rev_slow)
        + pump
        + exchange
    )
    new_x = x - (time_step / 100.0) * ionic
    new_calcium = calcium - (time_step * 0.05) * (calcium_sum - 2.0 * exchange)

    a = up5 * (e(7.0))
    b = power(1 / 200, -0.25)
    root = step(1 / 9.03, 56.86 / 9.03)
    rate = ((a * (-10.0 * speed) - (1.0 + e(-5.0)) * 10.0 * speed) - down5 * (e(-12.0) * 10.0 * speed)) * (
        (1.0 + b) * inverse(2.0 + a + b)
    )
    new_act = moved(act, root * root, rate)

    root = step(-1 / 7.43, -71.55 / 7.43)
    steady = root * root
    rate = minus_lower * (
        power(-1 / 6.8, -80.0 / 6.8, 0.057 * speed)
        + power(0.079, 0.0, 2.7 * speed)
        + power(0.3485, 0.0, 310000.0 * speed)
    ) + minus_upper * inverse(
        1.0 / (0.77 / 0.13 * speed) + power(-1 / 11.1, -10.66 / 11.1, 1.0 / (0.77 / 0.13 * speed))
    )
    new_inact = moved(inact, steady, rate)
    rate = minus_lower * (
        power(-0.01052, 0.0, 0.02424 * speed) * step(0.1378, 0.1378 * 40.14)
        - (power(0.2444, 0.0, 25428.0 * speed) + power(-0.04391, 0.0, 6.948e-06 * speed))
        * ((voltage + 37.78) * step(-0.311, -0.311 * 79.23))
    ) + minus_upper * (
        power(0.057) * inverse(1.0 / (0.6 * speed) + down10 * (e(-3.2) / (0.6 * speed)))
    )
    new_slow = moved(slow, steady, rate)

    p = 1.0 + power(-1 / 13, -35.0 / 13)
    r = down20 * (-speed * e(2.5)) - speed
    pq = p * (1.0 + up5 * e(1.0))
    rate = pq * (r * inverse((-1.96 / speed - (0.35 / speed) * p) * r + pq))
    new_calact = moved(calact, step(1 / 7.5, 8.0 / 7.5), rate)

    b = up10 * (-speed * e(3.0))
    den = (down10 * (-speed * e(1.3)) - speed * (1.0 + e(4.3))) + b
    rate = den * inverse(
        (380.0 - 180.0 * (1.0 + e(4.3)) - (20.0 / speed) * b)
        - (bell(27.0, 225.0, 1102.5 / speed) + 200.0 / speed) * den
    )
    new_calinact = moved(calinact, down7 * inverse(down7 + e(20.0 / 7)), rate)

    rate = inverse(-0.8 / speed - bell(40.0, 1800.0, 9.5 / speed))
    new_tract = moved(tract, inverse(1.0 + down6 * e(20.0 / 6)), rate)

    t = up5 * (-speed * e(-4.0)) - speed
    rate = t * inverse(5.0 - (bell(45.0, 320.0, 85.0 / speed) + 3.0 / speed) * t)
    new_trinact = moved(trinact, inverse(1.0 + up5 * e(4.0)), rate)

    rate = (down10 * (-speed * e(-4.5) / 2700.0) - speed / 2700.0) * (
        1.0 + power(1 / 11.5, 30.0 / 11.5)
    )
    new_rapact = moved(rapact, inverse(1.0 + down7 * e(-26.0 / 7)), rate)

    rate = (up20 + down20) * (-speed * e(-3.0) / 3.36) - speed * (1.0 + e(-6.0)) / 3.36
    new_rapinact = moved(rapinact, step(-1 / 24, -88.0 / 24), rate)

    y = up15 * (-speed * e(-35.0 / 15)) - speed
    rate = y * inverse(
        lax.rsqrt(1.0 / 1400.0**2 + down6 * (e(5.0 / 6) / 1400.0**2)) - (80.0 / speed) * y
    )
    new_slowact = moved(slowact, inverse(1.0 + down14 * e(-5.0 / 14)), rate)
    return (
        new_x,
        new_act,
        new_inact,
        new_slow,
        new_calact,
        new_calinact,
        new_tract,
        new_trinact,
        new_rapact,
        new_rapinact,
        new_slowact,
        new_calcium,
    )


def layer_tensor(layer_index, fibre):
    angle_in = fibre[0]
    angle_out = fibre[1]
    fibre_x = jnp.cos(angle_in) * jnp.cos(angle_out)
    fibre_y = jnp.sin(angle_in) * jnp.cos(angle_out)
    fibre_z = jnp.sin(angle_out)
    spread = longitudinal - transverse
    tensor_table = jnp.stack(
        [
            transverse + spread * fibre_x * fibre_x,
            transverse + spread * fibre_y * fibre_y,
            transverse + spread * fibre_z * fibre_z,
            spread * fibre_x * fibre_y,
            spread * fibre_x * fibre_z,
            spread * fibre_y * fibre_z,
        ]
    )
    layer_ids = jnp.arange(fibre.shape[1], dtype=jnp.int32)
    chosen = layer_index[:, None] == layer_ids[None, :]
    return jnp.sum(jnp.where(chosen[None], tensor_table[:, None, :], jnp.float32(0.0)), axis=2)


def level_weights(tensor, lanes):
    between = (tensor[:, 1:] + tensor[:, :-1]) / 2.0
    upward = jnp.pad(between, ((0, 0), (0, 1)))
    downward = jnp.pad(between, ((0, 0), (1, 0)))
    rows = jnp.stack(
        [
            tensor[0],
            tensor[1],
            tensor[3] / 2.0,
            upward[2],
            upward[4] / 2.0,
            upward[5] / 2.0,
            downward[2],
            downward[4] / 2.0,
            downward[5] / 2.0,
        ]
    )
    return jnp.broadcast_to(rows[:, :, None], rows.shape + (lanes,))


def first_kernel(chunks, state_ref, mask_ref, *refs):
    faces, (edge_ref, main, inside, sems) = refs[: 2 * len(chunks)], refs[2 * len(chunks) :]
    cells, depth, width = state_ref.shape[1:]
    odd = lax.rem(lax.axis_index("gx"), 2)
    lane = lax.broadcasted_iota(jnp.int32, (depth, LANES), 1)
    diagonal = lax.broadcasted_iota(jnp.int32, (depth, depth), 0) == lax.broadcasted_iota(
        jnp.int32, (depth, depth), 1
    )
    codes = jnp.zeros((depth, LANES), jnp.float32)
    for x in range(cells):
        for b in range(width // LANES):
            code = jnp.where(mask_ref[x, b : b + 1, :] > 0, jnp.float32(1.0), jnp.float32(0.0))
            code = jnp.where(diagonal, jnp.broadcast_to(code, (depth, depth)), jnp.float32(0.0))
            code = jnp.broadcast_to(jnp.sum(code, axis=1, keepdims=True), (depth, LANES))
            inside[x, :, pl.ds(b * LANES, LANES)] = code
            codes = jnp.where(lane == 2 * x + b, code, codes)
    edge_ref[COMPS + 1] = codes

    def react_pair(k, carry):
        for x in (2 * k, 2 * k + 1):
            for level in range(depth // 8):
                for i in range(width // LANES):
                    place = (x, pl.ds(level * 8, 8), pl.ds(i * LANES, LANES))
                    old = [state_ref[(c,) + place] for c in range(COMPS)]
                    live = inside[place] > 0.5
                    for c, new in enumerate(react(old)):
                        main[(c,) + place] = jnp.where(live, new, old[c])
        return carry

    lax.fori_loop(0, cells // 2, react_pair, 0)
    copies = []
    start = 0
    for i, rows in enumerate(chunks):
        above, below = cells - start - rows, start
        inner = above + odd * (below - above)
        outer = below + odd * (above - below)
        for face, row, sem in ((faces[2 * i], inner, 2 * i), (faces[2 * i + 1], outer, 2 * i + 1)):
            copies.append(pltpu.make_async_copy(main.at[:, pl.ds(row, rows)], face, sems.at[sem]))
        start += rows
    for copy in copies:
        copy.start()

    def packed(first, last):
        total = jnp.zeros((depth, LANES), jnp.float32)
        for i in range(cells):
            joined = jnp.where(lane < EDGE, first(i), last(i))
            turned = pltpu.roll(joined, i * GROUP + EDGE, 1)
            total = jnp.where(lane // GROUP == i, turned, total)
        return total

    def some(k, carry):
        for q in range(3):
            c = 3 * k + q
            edge_ref[c] = packed(
                lambda i: main[c, i, :, :LANES], lambda i: main[c, i, :, width - LANES :]
            )
        return carry

    lax.fori_loop(0, COMPS // 3, some, 0)
    edge_ref[COMPS] = packed(
        lambda i: inside[i, :, :LANES], lambda i: inside[i, :, width - LANES :]
    )
    for copy in copies:
        copy.wait()


def react_tile(at, live, kept=COMPS):
    new = react([at(c)[...] for c in range(COMPS)])
    for c in range(kept):
        pltpu.store(at(c), new[c], mask=live > 0.5)
    return live * new[0]


def react_rows(main, inside, pot, rows, kept=COMPS):
    for x in rows:
        for level in range(main.shape[2] // 8):
            for i in range(main.shape[3] // LANES):
                place = (x, pl.ds(level * 8, 8), pl.ds(i * LANES, LANES))
                pot[place] = react_tile(lambda c: main.at[(c,) + place], inside[place], kept)


def shift_row(pot, dy_ref, sy_ref, x, ext, strip_row):
    shape = (pot.shape[1], LANES)
    lane = lax.broadcasted_iota(jnp.int32, shape, 1)
    first_lane, last_lane = lane == 0, lane == LANES - 1
    block = pl.ds(pl.multiple_of(ext // 8 * LANES, LANES), LANES)
    place = lax.rem(ext, 8) * GROUP
    before = pltpu.roll(strip_row(0, block), lax.rem(2 * LANES - place - (EDGE - 1), LANES), 1)
    after = pltpu.roll(strip_row(1, block), lax.rem(2 * LANES - 1 - place - EDGE, LANES), 1)
    near, far = pot[x, :, :LANES], pot[x, :, LANES:]
    near_up, far_up = pltpu.roll(near, 1, 1), pltpu.roll(far, 1, 1)
    near_down, far_down = pltpu.roll(near, LANES - 1, 1), pltpu.roll(far, LANES - 1, 1)
    lower = jnp.where(first_lane, before, near_up)
    upper = jnp.where(last_lane, far_down, near_down)
    dy_ref[x, :, :LANES] = upper - lower
    sy_ref[x, :, :LANES] = upper + lower
    lower = jnp.where(first_lane, near_up, far_up)
    upper = jnp.where(last_lane, after, far_down)
    dy_ref[x, :, LANES:] = upper - lower
    sy_ref[x, :, LANES:] = upper + lower


def spread(weight_ref, p, dx, sx, dy, sy, cross):
    depth, lanes = p.shape
    w = [weight_ref[i, :, :lanes] for i in range(9)]
    rising = w[3] * p - w[4] * dx - w[5] * dy
    falling = w[6] * p + w[7] * dx + w[8] * dy
    return (
        w[0] * sx
        + w[1] * sy
        + w[2] * cross
        + pltpu.roll(rising, 1, 0)
        + pltpu.roll(falling, depth - 1, 0)
    )


def row_spread(weight_ref, pot, dy_ref, sy_ref, x):
    before, after = pot[x - 1], pot[x + 1]
    return spread(
        weight_ref,
        pot[x],
        after - before,
        after + before,
        dy_ref[x],
        sy_ref[x],
        dy_ref[x + 1] - dy_ref[x - 1],
    )


def strip_spread(weight_ref, p):
    long = p.shape[1]
    lower, upper = pltpu.roll(p, 1, 1), pltpu.roll(p, long - 1, 1)
    before, after = pltpu.roll(p, GROUP, 1), pltpu.roll(p, long - GROUP, 1)
    dy = upper - lower
    cross = pltpu.roll(dy, long - GROUP, 1) - pltpu.roll(dy, GROUP, 1)
    return spread(weight_ref, p, after - before, after + before, dy, upper + lower, cross)


def strip_kernel(
    strip_inner_hbm,
    strip_hbm,
    strip_outer_hbm,
    weight_ref,
    inside,
    total,
    strip_track,
    dy_ref,
    sy_ref,
    strip,
    code_ref,
    strip_total,
    sems,
):
    span, depth, width = inside.shape
    cells = span // 3
    odd = lax.rem(lax.axis_index("gx"), 2)
    sides = (0, 1)
    copies = []
    for q, (i, source) in enumerate(
        ((2 - 2 * odd, strip_inner_hbm), (1, strip_hbm), (2 * odd, strip_outer_hbm))
    ):
        part = pl.ds(pl.multiple_of(i * LANES, LANES), LANES)
        for side in sides:
            held = source.at[pl.ds(side * (COMPS + 1), COMPS + 1)]
            copies.append(
                pltpu.make_async_copy(held, strip.at[side, :, :, part], sems.at[3 * q + side])
            )
        copies.append(
            pltpu.make_async_copy(
                source.at[pl.ds(2 * (COMPS + 1), 1)], code_ref.at[pl.ds(i, 1)], sems.at[3 * q + 2]
            )
        )
    for copy in copies:
        copy.start()
    for copy in copies:
        copy.wait()
    for i in range(3):
        codes = code_ref[i]
        for x in range(cells):
            for b in range(width // LANES):
                value = jnp.broadcast_to(codes[:, 2 * x + b : 2 * x + b + 1], (depth, LANES))
                inside[i * cells + x, :, b * LANES : (b + 1) * LANES] = value

    def shift_mask(k, carry):
        for q in range(4):
            x = 4 * k + q
            shift_row(inside, dy_ref, sy_ref, x, x, lambda side, block: strip[side, COMPS, :, block])
        return carry

    lax.fori_loop(0, span // 4, shift_mask, 0)

    def total_rows(k, carry):
        for q in range(2):
            x = 1 + 2 * k + q
            total[x] = row_spread(weight_ref, inside, dy_ref, sy_ref, x)
        return carry

    lax.fori_loop(0, span // 2 - 1, total_rows, 0)
    for side in sides:
        strip_total[side] = strip_spread(weight_ref, strip[side, COMPS])
        strip_track[0, side] = strip[side, COMPS] * strip[side, 0]

    def step(kept, s, carry):
        for side in sides:
            u = strip[side, 0]
            flow = strip_spread(weight_ref, strip_track[s, side]) - u * strip_total[side]
            strip[side, 0] = u + strip[side, COMPS] * flow

        for side in sides:
            for level in range(depth // 8):
                for i in range(3):
                    place = (pl.ds(level * 8, 8), pl.ds(i * LANES, LANES))
                    held = react_tile(
                        lambda c: strip.at[(side, c) + place], strip[(side, COMPS) + place], kept
                    )
                    strip_track[(s + 1, side) + place] = held
        return carry

    lax.fori_loop(0, STEPS - 2, functools.partial(step, COMPS), 0)
    step(1, STEPS - 2, 0)


def finished(main, main_out, sems, s, wait):
    count = main.shape[1]
    for q, row in enumerate((s, count - 1 - s)):
        copy = pltpu.make_async_copy(
            main.at[:, pl.ds(row, 1)], main_out.at[:, pl.ds(row, 1)], sems.at[2 * s + q]
        )
        if wait:
            copy.wait()
        else:
            copy.start()


def in_two(source, main, row, sems, i):
    place = pl.ds(row, source.shape[1])
    return [
        pltpu.make_async_copy(source.at[part], main.at[part, place], sems.at[2 * i + q])
        for q, part in enumerate((pl.ds(0, 1), pl.ds(1, COMPS - 1)))
    ]


def near_kernel(pieces, near, *refs):
    sources, refs = refs[: pieces + 2], refs[pieces + 2 :]
    inside, total, strip_track, weight_ref, main_out, track = refs[:6]
    main, pot, dy_ref, sy_ref, sems, out_sems = refs[6:]
    count, _, _ = pot.shape
    cells = count - 2 * near
    skip = cells - near
    odd = lax.rem(lax.axis_index("gx"), 2)
    inner_hbm, outer_hbm = sources[:2]
    places = [(near + cells - odd * (near + cells), inner_hbm), (odd * (near + cells), outer_hbm)]
    start = 0
    for source in sources[2:]:
        rows = source.shape[1]
        above, below = cells - start - rows, start
        places.append((near + above + odd * (below - above), source))
        start += rows
    copies = [in_two(source, main, row, sems, i) for i, (row, source) in enumerate(places)]
    for part in range(2):
        for copy in copies:
            copy[part].start()
    for copy in copies:
        copy[0].wait()

    group = 4 if count % 4 == 0 else 2

    def start_row(k, carry):
        for q in range(2):
            pot[2 * k + q] = inside[skip + 2 * k + q] * main[0, 2 * k + q]
        return carry

    lax.fori_loop(0, count // 2, start_row, 0)

    def shift(s, x):
        shift_row(
            pot, dy_ref, sy_ref, x, skip + x, lambda side, block: strip_track[s, side, :, block]
        )

    def shift_some(k, carry):
        for q in range(group):
            shift(0, group * k + q)
        return carry

    lax.fori_loop(0, count // group, shift_some, 0)

    def step(s, carry):
        for q, row in enumerate((s + 1, count - 2 - s)):
            track[s, q, 0] = pot[row]
            track[s, q, 1] = dy_ref[row]

        def diffuse_some(size, start, k, carry):
            for q in range(size):
                x = start + size * k + q
                u = main[0, x]
                flow = row_spread(weight_ref, pot, dy_ref, sy_ref, x) - u * total[skip + x]
                main[0, x] = u + inside[skip + x] * flow
            return carry

        pairs = jnp.maximum(count // 2 - 1 - s, 0)
        lax.fori_loop(0, pairs // 2, functools.partial(diffuse_some, 4, s + 1), 0)
        rest = s + 1 + pairs // 2 * 4
        lax.fori_loop(0, lax.rem(pairs, 2), functools.partial(diffuse_some, 2, rest), 0)

        @pl.when(s == 0)
        def _():
            for copy in copies:
                copy[1].wait()

        @pl.when(s < min(STEPS, count // 2))
        def _():
            finished(main, main_out, out_sems, s, False)

        def react_some(k, carry):
            x = s + 1 + 2 * k
            for q in range(2):
                shift(s + 1, jnp.maximum(x - 2 + q, 0))
            react_rows(main, inside.at[pl.ds(skip, count)], pot, (x, x + 1))
            return carry

        @pl.when(s < min(STEPS - 1, count // 2 - 1))
        def _():
            lax.fori_loop(0, count // 2 - 1 - s, react_some, 0)
            for q in range(2):
                shift(s + 1, count - 3 - s + q)

        return carry

    lax.fori_loop(0, STEPS, step, 0)

    def drained(s, carry):
        finished(main, main_out, out_sems, s, True)
        return carry

    lax.fori_loop(0, min(STEPS, count // 2), drained, 0)


def ring_kernel(last, *refs):
    inner_hbm, main_hbm, outer_hbm, relay_hbm = refs[:4]
    inside, total, strip_track, track, weight_ref = refs[4:9]
    if last:
        out_hbm, main, pot, dy_ref, sy_ref, sems = refs[9:]
    else:
        main_out, track_out, main, pot, dy_ref, sy_ref, sems, out_sems = refs[9:]
    far, _, _ = inner_hbm.shape[1:]
    count = main_hbm.shape[1]
    span = far + count + far
    cells = inside.shape[0] // 3
    skip = (inside.shape[0] - span) // 2
    before = (count - cells) // 2
    odd = lax.rem(lax.axis_index("gx"), 2)
    across = lax.rem(lax.axis_index("gx") + 1, PLANE)
    relayed = jnp.logical_or(across == 0, across == 1)
    inner_place, outer_place = far + count - odd * (far + count), odd * (far + count)
    copies = [
        pltpu.make_async_copy(source, main.at[:, pl.ds(row, source.shape[1])], sems.at[i])
        for i, (row, source) in enumerate(
            (
                (inner_place, inner_hbm),
                (far, main_hbm),
                (outer_place, relay_hbm),
                (outer_place, outer_hbm),
            )
        )
    ]
    copies[0].start()
    copies[1].start()

    @pl.when(relayed)
    def _():
        copies[2].start()
        copies[2].wait()

    @pl.when(jnp.logical_not(relayed))
    def _():
        copies[3].start()
        copies[3].wait()

    copies[0].wait()
    copies[1].wait()
    for q in range(far):
        for x in (q, span - 1 - q):
            pot[x] = inside[skip + x] * main[0, x]

    def shift(s, x):
        shift_row(
            pot, dy_ref, sy_ref, x, skip + x, lambda side, block: strip_track[s, side, :, block]
        )

    for q in range(far - 1):
        for x in (q, span - 1 - q):
            shift(0, x)

    def step(s, carry):
        for row in (s + far, span - 1 - far - s):
            pot[row] = inside[skip + row] * main[0, row]
        for q in (far - 1, far):
            for x in (s + q, span - 1 - s - q):
                shift(s, x)

        def known():
            for q, row in enumerate((s + far + 1, span - 2 - far - s)):
                pot[row] = track[s, q, 0]
                dy_ref[row] = track[s, q, 1]

        if before < cells // 2:
            pl.when(s < cells // 2 + before)(known)
        else:
            known()
        if not last:
            for q, row in enumerate((s + 1, span - 2 - s)):
                track_out[s, q, 0] = pot[row]
                track_out[s, q, 1] = dy_ref[row]

        def diffuse(x):
            u = main[0, x]
            flow = row_spread(weight_ref, pot, dy_ref, sy_ref, x) - u * total[skip + x]
            main[0, x] = u + inside[skip + x] * flow

        for side, first in enumerate((s + 1, span - 1 - far - s)):
            for q in range(far):
                x = first + q
                if before < cells // 2 and q == (far - 1, 0)[side]:
                    pl.when((x < span // 2, x >= span // 2)[side])(functools.partial(diffuse, x))
                else:
                    diffuse(x)
        if not last:
            finished(main, main_out, out_sems, s, False)

        held = inside.at[pl.ds(skip, span)]

        def react_pair(k, carry):
            near_row, far_row = s + 1 + k, span - 2 - s - k
            shift(s + 1, near_row - 1)
            shift(s + 1, far_row + 1)
            react_rows(main, held, pot, (near_row, far_row))
            return carry

        @pl.when(s < STEPS - 1)
        def _():
            react_rows(main, held, pot, (s + 1, span - 2 - s), 1 if last else COMPS)
            lax.fori_loop(1, far, react_pair, 0)

        return carry

    lax.fori_loop(0, STEPS, step, 0)
    if last:
        copies = [pltpu.make_async_copy(main.at[:, pl.ds(cells, cells)], out_hbm, sems.at[0])]
    else:
        rest = span - 2 * STEPS
        copies = [
            pltpu.make_async_copy(
                main.at[:, pl.ds(STEPS, rest)], main_out.at[:, pl.ds(STEPS, rest)], sems.at[0]
            )
        ] * (rest > 0)
    for copy in copies:
        copy.start()
    for copy in copies:
        copy.wait()
    if not last:

        def drained(s, carry):
            finished(main, main_out, out_sems, s, True)
            return carry

        lax.fori_loop(0, STEPS, drained, 0)


def shards(state, tissue_mask, layer_index, fibre):
    comps, cells, depth, width = state.shape
    across, along = lax.axis_size("gx"), lax.axis_size("gy")
    span = 3 * cells
    f32 = jnp.float32

    def swaps(size, first):
        pairs = [(i, i + 1) for i in range(first, size - 1, 2)]
        return pairs + [(j, i) for i, j in pairs]

    def both(inner, outer, axis, size):
        outer = lax.ppermute(outer, axis, swaps(size, 1))
        return lax.ppermute(inner, axis, swaps(size, 0)), outer

    def shape(*sizes):
        return jax.ShapeDtypeStruct(sizes, f32)

    vmem = pl.BlockSpec(memory_space=pltpu.VMEM)
    hbm = pl.BlockSpec(memory_space=pl.ANY)
    params = pltpu.CompilerParams(vmem_limit_bytes=12 << 20)

    def cost(rows):
        work = int(rows * depth * width * 350)
        return pl.CostEstimate(flops=work, bytes_accessed=8 << 20, transcendentals=0)

    *faces, edge = pl.pallas_call(
        functools.partial(first_kernel, CHUNKS),
        out_shape=[shape(comps, rows, depth, width) for rows in CHUNKS for _ in range(2)]
        + [shape(comps + 2, depth, LANES)],
        in_specs=[vmem, vmem],
        out_specs=[hbm] * (2 * len(CHUNKS)) + [vmem],
        scratch_shapes=[
            pltpu.VMEM((comps, cells, depth, width), f32),
            pltpu.VMEM((cells, depth, width), f32),
            pltpu.SemaphoreType.DMA((2 * len(CHUNKS),)),
        ],
        compiler_params=params,
        name="first",
    )(state, tissue_mask.transpose(0, 2, 1))
    inner_faces, outer_faces = faces[0::2], faces[1::2]
    edge_inner, edge_outer = both(edge, edge, "gy", along)
    odd_along = lax.rem(lax.axis_index("gy"), 2) == 1
    edge_before = jnp.where(odd_along, edge_inner, edge_outer)
    edge_after = jnp.where(odd_along, edge_outer, edge_inner)
    outer = lax.broadcasted_iota(jnp.int32, edge.shape, 2) % GROUP < EDGE
    strips = jnp.concatenate(
        [
            jnp.where(outer, edge_before, edge)[:-1],
            jnp.where(outer, edge, edge_after)[:-1],
            edge[-1:],
        ]
    )
    strip_inner, strip_outer = both(strips, strips, "gx", across)
    halos = [both(inner_faces[0], outer_faces[0], "gx", across)]
    bounds = [i for i in range(PLANE - 1, across - 1, PLANE)]
    close = [pair for pair in swaps(across, 1) if pair[0] // PLANE == pair[1] // PLANE]
    around = [(i, i - PLANE + 1) for i in bounds] + [(i + 1, i + PLANE) for i in bounds]
    onward = [(i - PLANE + 1, i + 1) for i in bounds] + [(i + PLANE, i) for i in bounds]
    far_outer = lax.ppermute(outer_faces[1], "gx", close + around)
    far_inner = lax.ppermute(inner_faces[1], "gx", swaps(across, 0))
    far_relay = lax.ppermute(far_outer, "gx", onward)
    halos.append((far_inner, far_outer, far_relay))

    weights = level_weights(layer_tensor(layer_index, fibre), 3 * LANES)
    inside, total, strip_track = pl.pallas_call(
        strip_kernel,
        out_shape=[
            shape(span, depth, width),
            shape(span, depth, width),
            shape(STEPS, 2, depth, 3 * LANES),
        ],
        in_specs=[hbm] * 3 + [vmem],
        out_specs=[vmem] * 3,
        scratch_shapes=[
            pltpu.VMEM((span, depth, width), f32),
            pltpu.VMEM((span, depth, width), f32),
            pltpu.VMEM((2, comps + 1, depth, 3 * LANES), f32),
            pltpu.VMEM((3, depth, LANES), f32),
            pltpu.VMEM((2, depth, 3 * LANES), f32),
            pltpu.SemaphoreType.DMA((9,)),
        ],
        compiler_params=params,
        cost_estimate=cost(30),
        name="strips",
    )(strip_inner, strips, strip_outer, weights)
    shared = (inside, total, strip_track)

    def buffers(count):
        return [pltpu.VMEM((comps, count, depth, width), f32)] + [
            pltpu.VMEM((count, depth, width), f32) for _ in range(3)
        ]

    track_shape = shape(STEPS, 2, 2, depth, width)
    near = CHUNKS[0]
    count = cells + 2 * near
    main, track = pl.pallas_call(
        functools.partial(near_kernel, len(CHUNKS), near),
        out_shape=[shape(comps, count, depth, width), track_shape],
        in_specs=[hbm] * (2 + len(CHUNKS)) + [vmem] * 4,
        out_specs=[hbm, vmem],
        scratch_shapes=buffers(count)
        + [pltpu.SemaphoreType.DMA((2 * (2 + len(CHUNKS)),)), pltpu.SemaphoreType.DMA((2 * STEPS,))],
        compiler_params=params,
        cost_estimate=cost(70),
        name="near",
    )(*halos[0], *inner_faces, *shared, weights)
    for i, rows in enumerate(CHUNKS[1:], 1):
        last = i == len(CHUNKS) - 1
        count += 2 * rows
        outs = [shape(*state.shape)] if last else [shape(comps, count, depth, width), track_shape]
        result = pl.pallas_call(
            functools.partial(ring_kernel, last),
            out_shape=outs,
            in_specs=[hbm] * 4 + [vmem] * 5,
            out_specs=[hbm, vmem][: len(outs)],
            scratch_shapes=buffers(count)
            + [pltpu.SemaphoreType.DMA((4,))]
            + ([] if last else [pltpu.SemaphoreType.DMA((2 * STEPS,))]),
            compiler_params=params,
            cost_estimate=cost(18 * rows),
        )(halos[i][0], main, *halos[i][1:], *shared, track, weights)
        main, track = result if not last else (result[0], None)
    return main


def solution(mesh):
    placed = (P(None, "gx", None, "gy"), P("gx", None, "gy"), P(), P())

    return jax.shard_map(
        shards, mesh=mesh, in_specs=placed, out_specs=P(None, "gx", None, "gy"), check_vma=False
    )
```
